512 devices in a mesh: dp: 128 (over z_lo, y, x, core), mp: 4 (over z_hi).
Axes of the slice: x: 4, y: 8, z: 8 (z_hi: 4, z_lo: 2; z = z_hi * 2 + z_lo), core: 2. Of those that a mesh axis runs over, the one named last changes fastest.
Arguments:
- feature_ids: int32 [16384, 128], P('dp'), may hold values from 0 to 8191
- emb_table: bfloat16 [8192, 128], P(('dp', 'mp')), may hold values from -6 to 6
- factor_machine_projection: bfloat16 [128, 32], replicated, may hold values from -0.5 to 0.5
- mlp_weight: float32 [4096, 1024], P('dp', 'mp'), may hold values from -0.09375 to 0.09375
- momentum: float32 [4096, 1024], P('dp', 'mp'), may hold values from -6 to 6
- hidden_grad: bfloat16 [16384, 1024], P('dp', 'mp'), may hold values from -0.125 to 0.125
- lcb_grad: bfloat16 [16384, 128, 128], P('dp', 'mp'), may hold values from -0.009765625 to 0.009765625
Outputs:
- new_weight: float32 [4096, 1024], P('dp', 'mp')
- new_momentum: float32 [4096, 1024], P('dp', 'mp')
- next_weight: bfloat16 [4096, 1024], P(None, 'mp')
- proj_grad: float32 [128, 32], replicated
- lcb_weight_grad: float32 [128, 128], P(None, 'mp')
The draws below stay inside these ranges and needn't reach their ends.
All inputs are finite; a program needn't handle non-finite values.
Results may differ from the reference program's by a relative error of at most 0.0074.
Values may be sent and summed in bfloat16 or wider, within the bound.
No kernel may reach another device: no remote copies, remote signals or barrier semaphores. Data moves between devices by JAX's collectives and lax.ppermute only.
A program may use at most 64 MiB of HBM per device.

```python
import jax
import jax.numpy as jnp
from jax import lax

D = 128
EMBEDDING_COUNT = 128
COMPRESS_RANK = 32
HID = 1024
NL = 128
EXAMPLES_PER_DP = 128
BATCH = 16384
IN = 4096
VOCAB = 8192


def place_ends(drawn, stream_key, smallest, top_value):
    extent = drawn.shape
    place = [jax.random.randint(jax.random.fold_in(stream_key, axis), (), 0, extent[axis]) for axis in range(len(extent))]
    drawn = drawn.at[tuple(place)].set(smallest)
    longest = extent.index(max(extent))
    place[longest] = (place[longest] + 1) % extent[longest]
    return drawn.at[tuple(place)].set(top_value)


def block_scale(stream_key, shape, shards, smallest, top_value):
    factor_of = 1.0
    for position, parts in shards:
        steps = jax.random.uniform(jax.random.fold_in(jax.random.fold_in(stream_key, 6), position), (parts,), jnp.float32, smallest / len(shards), top_value / len(shards))
        factor_of = factor_of * jnp.repeat(jnp.exp(steps), shape[position] // parts).reshape((-1,) + (1,) * (len(shape) - 1 - position))
    return factor_of


def gaussian(rng, extent, spread, most, cuts=(), kind=jnp.bfloat16):
    gain = block_scale(rng, extent, cuts, -0.22, 0.18) if cuts else 1.0
    array = jax.random.normal(rng, extent, jnp.float32) * spread * gain
    return jnp.minimum(jnp.maximum(array, -most), most).astype(kind)


def setup_inputs(seed: int = 0) -> dict:
    key_of = jax.random.split(jax.random.key(seed), 8)
    feature_ids = place_ends(jax.random.randint(key_of[0], (BATCH, EMBEDDING_COUNT), 0, VOCAB), jax.random.fold_in(key_of[0], 1), 0, VOCAB - 1).astype(jnp.int32)
    emb_table = gaussian(key_of[1], (VOCAB, D), 1.0, 6.0, ((0, 512),))
    factor_machine_projection = gaussian(key_of[2], (EMBEDDING_COUNT, COMPRESS_RANK), EMBEDDING_COUNT ** -0.5, 0.5)
    mlp_weight = gaussian(key_of[3], (IN, HID), IN ** -0.5, 0.09375, ((0, 128), (1, 4)), jnp.float32)
    momentum = gaussian(key_of[4], (IN, HID), 1.0, 6.0, ((0, 128), (1, 4)), jnp.float32)
    hidden_grad = gaussian(key_of[5], (BATCH, HID), (BATCH ** -0.5), 0.125, ((0, 128), (1, 4)))
    lcb_grad = gaussian(key_of[6], (BATCH, NL, D), ((BATCH * D) ** -0.5), 0.009765625, ((0, 128), (1, 4)))
    return {"feature_ids": feature_ids, "emb_table": emb_table, "factor_machine_projection": factor_machine_projection, "mlp_weight": mlp_weight, "momentum": momentum, "hidden_grad": hidden_grad, "lcb_grad": lcb_grad}


def reference(feature_ids, emb_table, factor_machine_projection, mlp_weight, momentum, hidden_grad, lcb_grad):
    weight_bf = mlp_weight.astype(jnp.bfloat16)
    projection_float = factor_machine_projection.astype(jnp.float32)
    blocks = feature_ids.shape[0] // EXAMPLES_PER_DP

    def step_block(totals, block_index):
        grad_total, projection_gradient_total, lcb_total = totals
        begin_row = (block_index * EXAMPLES_PER_DP).astype(jnp.int32)
        ids_block = lax.dynamic_slice_in_dim(feature_ids, begin_row, EXAMPLES_PER_DP, 0)
        cot_block = lax.dynamic_slice_in_dim(hidden_grad, begin_row, EXAMPLES_PER_DP, 0)
        lcb_block = lax.dynamic_slice_in_dim(lcb_grad, begin_row, EXAMPLES_PER_DP, 0)
        embedded_rows = jnp.take(emb_table, ids_block, axis=0).astype(jnp.float32)
        lcb_total = lcb_total + jnp.einsum('bnd,bld->nl', embedded_rows, lcb_block.astype(jnp.float32))
        compressed_rows = jnp.einsum('fpy,po->foy', embedded_rows, projection_float).astype(jnp.bfloat16)
        factor_machine_output = jnp.einsum('cqr,cor->cqo', compressed_rows.astype(jnp.float32), embedded_rows).reshape(EXAMPLES_PER_DP, COMPRESS_RANK * EMBEDDING_COUNT)
        row_mean = lax.optimization_barrier(jnp.mean(factor_machine_output, axis=1, keepdims=True))
        centered = factor_machine_output - row_mean
        row_var = lax.optimization_barrier(jnp.mean(centered * centered, axis=1, keepdims=True))
        inv_scale = 1.0 / jnp.sqrt(row_var + 1.0)
        normed = centered * inv_scale
        normed_bf = normed.astype(jnp.bfloat16)
        preact = jnp.dot(normed_bf, weight_bf, preferred_element_type=jnp.float32)
        sigmoid_pre = jax.nn.sigmoid(preact)
        preact_grad = (cot_block.astype(jnp.float32) * sigmoid_pre * (1.0 + preact * (1.0 - sigmoid_pre))).astype(jnp.bfloat16)
        grad_total = grad_total + jnp.dot(normed_bf.T, preact_grad, preferred_element_type=jnp.float32)
        normed_grad = jnp.dot(preact_grad, weight_bf.T, preferred_element_type=jnp.float32)
        factor_machine_gradient = (normed_grad - lax.optimization_barrier(jnp.mean(normed_grad, axis=1, keepdims=True)) - normed * lax.optimization_barrier(jnp.mean(normed_grad * normed, axis=1, keepdims=True))) * inv_scale
        factor_machine_gradient = factor_machine_gradient.astype(jnp.bfloat16).reshape(EXAMPLES_PER_DP, COMPRESS_RANK, EMBEDDING_COUNT).astype(jnp.float32)
        projection_backprop = jnp.einsum('soe,sez->soz', factor_machine_gradient, embedded_rows).astype(jnp.bfloat16)
        projection_gradient_total = projection_gradient_total + jnp.einsum('jlh,jqh->lq', embedded_rows, projection_backprop.astype(jnp.float32))
        return ((grad_total, projection_gradient_total, lcb_total), None)
    start_totals = (jnp.zeros((EMBEDDING_COUNT * COMPRESS_RANK, HID), jnp.float32), jnp.zeros((EMBEDDING_COUNT, COMPRESS_RANK), jnp.float32), jnp.zeros((EMBEDDING_COUNT, NL), jnp.float32))
    totals, _ = lax.scan(step_block, start_totals, jnp.arange(blocks).astype(jnp.int32))
    weight_grad, proj_grad, lcb_weight_grad = totals
    new_momentum = 0.9 * momentum + weight_grad
    new_weight = mlp_weight - 0.01 * new_momentum
    next_weight = new_weight.astype(jnp.bfloat16)
    return (new_weight, new_momentum, next_weight, proj_grad, lcb_weight_grad)
```

```python
import jax
import jax.numpy as jnp
from jax import lax
from jax.experimental import pallas as pl
from jax.experimental.pallas import tpu as pltpu
from jax.sharding import Mesh
from jax.sharding import PartitionSpec as P

DP = ("zl", "y", "x", "c")
DP_MP = ("zl", "y", "x", "c", "mp")
GROUP = 8


def exchange(tiles, axis):
    return lax.all_to_all(tiles, axis, split_axis=0, concat_axis=0, tiled=True)


def from_everyone(x, axis):
    return exchange(jnp.broadcast_to(x, (lax.axis_size(axis), *x.shape)), axis)


def summed(tiles):
    return tiles.astype(jnp.float32).sum(axis=0)


def forward_kernel(ids_ref, table_ref, proj_ref, emb_ref, normed_ref, inv_ref, even_ref, odd_ref, fm_ref):
    rank, n_emb = proj_ref.shape
    proj = proj_ref[...]
    for e in range(GROUP):
        rows_ref = (even_ref, odd_ref)[e % 2]
        for r in range(n_emb):
            rows_ref[pl.ds(r, 1), :] = table_ref[ids_ref[e, r]]
        emb = rows_ref[...].astype(jnp.bfloat16)
        emb_ref[e] = emb
        compressed = jnp.dot(proj, emb, preferred_element_type=jnp.float32).astype(jnp.bfloat16)
        fm_ref[pl.ds(e * rank, rank), :] = lax.dot_general(
            compressed, emb, (((1,), (1,)), ((), ())), preferred_element_type=jnp.float32
        )
    scale = 1.0 / (rank * n_emb)
    parts = [fm_ref[pl.ds(k, GROUP, stride=rank), :] for k in range(rank)]
    mean = jnp.sum(sum(parts), axis=1, keepdims=True) * scale
    parts = [p - mean for p in parts]
    var = jnp.sum(sum(p * p for p in parts), axis=1, keepdims=True) * scale
    inv = 1.0 / jnp.sqrt(var + 1.0)
    for k in range(rank):
        normed_ref[:, k * n_emb : (k + 1) * n_emb] = (parts[k] * inv).astype(jnp.bfloat16)
    inv_ref[...] = jnp.broadcast_to(inv, inv_ref.shape)


def forward_features(ids, table, projection):
    examples, n_emb = ids.shape
    vocab, width = table.shape
    rank = projection.shape[1]
    rows = table.astype(jnp.float32).reshape(vocab, 1, width)
    return pl.pallas_call(
        forward_kernel,
        grid=(examples // GROUP,),
        in_specs=[
            pl.BlockSpec((GROUP, n_emb), lambda g: (g, 0), memory_space=pltpu.SMEM),
            pl.BlockSpec((vocab, 1, width), lambda g: (0, 0, 0)),
            pl.BlockSpec((rank, n_emb), lambda g: (0, 0)),
        ],
        out_specs=[
            pl.BlockSpec((GROUP, n_emb, width), lambda g: (g, 0, 0)),
            pl.BlockSpec((GROUP, rank * n_emb), lambda g: (g, 0)),
            pl.BlockSpec((GROUP, 128), lambda g: (g, 0)),
        ],
        out_shape=[
            jax.ShapeDtypeStruct((examples, n_emb, width), jnp.bfloat16),
            jax.ShapeDtypeStruct((examples, rank * n_emb), jnp.bfloat16),
            jax.ShapeDtypeStruct((examples, 128), jnp.float32),
        ],
        scratch_shapes=[
            pltpu.VMEM((n_emb, width), jnp.float32),
            pltpu.VMEM((n_emb, width), jnp.float32),
            pltpu.VMEM((GROUP * rank, n_emb), jnp.float32),
        ],
        cost_estimate=pl.CostEstimate(
            flops=64 * examples * rank * n_emb * width,
            bytes_accessed=vocab * width * 4 + examples * n_emb * width * 2,
            transcendentals=0,
        ),
        name="fm_forward",
    )(ids, rows, projection.T)


def backward_kernel(grad_ref, normed_ref, inv_ref, emb_ref, out_ref, fm_grad_ref):
    n_emb = emb_ref.shape[1]
    rank = out_ref.shape[0]

    @pl.when(pl.program_id(0) == 0)
    def _():
        out_ref[...] = jnp.zeros_like(out_ref)

    def cut(ref, k):
        return ref[:, k * n_emb : (k + 1) * n_emb].astype(jnp.float32)

    scale = 1.0 / (rank * n_emb)
    grads = [cut(grad_ref, k) for k in range(rank)]
    normed = [cut(normed_ref, k) for k in range(rank)]
    mean = jnp.sum(sum(grads), axis=1, keepdims=True) * scale
    along = jnp.sum(sum(g * x for g, x in zip(grads, normed)), axis=1, keepdims=True) * scale
    inv = inv_ref[:, :1]
    for k in range(rank):
        fm_grad_ref[pl.ds(k, GROUP, stride=rank), :] = (grads[k] - mean - normed[k] * along) * inv
    total = jnp.zeros(out_ref.shape, jnp.float32)
    for e in range(GROUP):
        fm_grad = fm_grad_ref[pl.ds(e * rank, rank), :].astype(jnp.bfloat16)
        emb = emb_ref[e]
        back = jnp.dot(fm_grad, emb, preferred_element_type=jnp.float32).astype(jnp.bfloat16)
        total += lax.dot_general(back, emb, (((1,), (1,)), ((), ())), preferred_element_type=jnp.float32)
    out_ref[...] += total


def backward_features(normed_grad, normed, inv_scale, embedded, rank):
    examples, n_emb, width = embedded.shape
    return pl.pallas_call(
        backward_kernel,
        grid=(examples // GROUP,),
        in_specs=[
            pl.BlockSpec((GROUP, rank * n_emb), lambda g: (g, 0)),
            pl.BlockSpec((GROUP, rank * n_emb), lambda g: (g, 0)),
            pl.BlockSpec((GROUP, 128), lambda g: (g, 0)),
            pl.BlockSpec((GROUP, n_emb, width), lambda g: (g, 0, 0)),
        ],
        out_specs=pl.BlockSpec((rank, n_emb), lambda g: (0, 0)),
        out_shape=jax.ShapeDtypeStruct((rank, n_emb), jnp.float32),
        scratch_shapes=[pltpu.VMEM((GROUP * rank, n_emb), jnp.float32)],
        cost_estimate=pl.CostEstimate(
            flops=24 * examples * rank * n_emb * width,
            bytes_accessed=examples * n_emb * (width * 2 + rank * 6),
            transcendentals=0,
        ),
        name="fm_backward",
    )(normed_grad, normed, inv_scale, embedded)


def rows_from_group(rows):
    return from_everyone(from_everyone(from_everyone(rows, ("zl", "y")), "x"), "c")


def in_row_order(tiles):
    c, x, zy, rows, width = tiles.shape
    return jnp.transpose(tiles, (2, 1, 0, 3, 4)).reshape(zy * x * c * rows, width)


def sum_at_row_owner(part):
    x, c, zy = lax.axis_size("x"), lax.axis_size("c"), lax.axis_size(("zl", "y"))
    width = part.shape[1]
    tiles = jnp.transpose(part.reshape(zy, x, c, -1, width), (2, 1, 0, 3, 4))
    tiles = summed(exchange(tiles, "c")).astype(jnp.bfloat16)
    tiles = summed(exchange(tiles, "x")).astype(jnp.bfloat16)
    return summed(exchange(tiles, ("zl", "y")))


def per_device(feature_ids, emb_table, factor_machine_projection, mlp_weight, momentum, hidden_grad, lcb_grad):
    mp, zl, y, x, c = (lax.axis_size(a) for a in ("mp", "zl", "y", "x", "c"))
    own = emb_table.shape[0]
    rank = factor_machine_projection.shape[1]

    table = from_everyone(from_everyone(from_everyone(emb_table, ("mp", "zl", "y")), "x"), "c")
    table = table.reshape(-1, emb_table.shape[1])
    owner, row = feature_ids // own, feature_ids % own
    owner, at_mp = owner // mp, owner % mp
    owner, at_c = owner // c, owner % c
    at_zy, at_x = owner // x, owner % x
    ids = (((at_c * x + at_x) * mp + at_mp) * (zl * y) + at_zy) * own + row

    weights = in_row_order(rows_from_group(mlp_weight.astype(jnp.bfloat16)))
    embedded, normed, inv_scale = forward_features(ids, table, factor_machine_projection)
    preact = jnp.dot(normed, weights, preferred_element_type=jnp.float32)
    sigmoid_pre = jax.nn.sigmoid(preact)
    preact_grad = (
        hidden_grad.astype(jnp.float32) * sigmoid_pre * (1.0 + preact * (1.0 - sigmoid_pre))
    ).astype(jnp.bfloat16)
    weight_grad = sum_at_row_owner(
        lax.dot_general(
            normed, preact_grad, (((0,), (0,)), ((), ())), preferred_element_type=jnp.float32
        ).astype(jnp.bfloat16)
    )
    new_momentum = 0.9 * momentum + weight_grad
    new_weight = mlp_weight - 0.01 * new_momentum
    next_weight = in_row_order(rows_from_group(new_weight.astype(jnp.bfloat16)))

    normed_part = lax.dot_general(
        preact_grad, weights, (((1,), (1,)), ((), ())), preferred_element_type=jnp.float32
    )
    proj_part = backward_features(normed_part, normed, inv_scale, embedded, rank)
    lcb_part = jnp.einsum("bld,bnd->ln", lcb_grad, embedded, preferred_element_type=jnp.float32)
    n_emb = lcb_part.shape[1]
    both = jnp.concatenate(
        [proj_part.reshape(x * c, -1, n_emb), lcb_part.reshape(x * c, -1, n_emb)], axis=1
    )
    each = rank // (x * c)
    both = summed(exchange(both, ("x", "c")))
    both = summed(from_everyone(both, ("zl", "y")))
    proj_sum = summed(from_everyone(both[:each], "mp"))
    both = from_everyone(jnp.concatenate([proj_sum, both[each:]], axis=0), ("x", "c"))
    proj_grad = both[:, :each].reshape(-1, n_emb).T
    lcb_weight_grad = both[:, each:].reshape(-1, n_emb).T
    return (new_weight, new_momentum, next_weight, proj_grad, lcb_weight_grad)


def solution(mesh):
    torus = Mesh(mesh.devices.reshape(2, 8, 4, 2, mesh.shape["mp"]), DP_MP)
    placed = (
        P(DP, None),
        P(DP_MP, None),
        P(),
        P(DP, "mp"),
        P(DP, "mp"),
        P(DP, "mp"),
        P(DP, "mp", None),
    )
    return jax.shard_map(
        per_device,
        mesh=torus,
        in_specs=placed,
        out_specs=(P(DP, "mp"), P(DP, "mp"), P(None, "mp"), P(), P(None, "mp")),
        check_vma=False,
    )
```

```python
import jax
import jax.numpy as jnp
from jax import lax
from jax.experimental import pallas as pl
from jax.experimental.pallas import tpu as pltpu
from jax.sharding import Mesh
from jax.sharding import PartitionSpec as P


DP = ("zl", "y", "x", "c")
DP_MP = ("zl", "y", "x", "c", "mp")
CX = ("c", "x")
ZY = ("zl", "y")
GROUP = 8
FIRST_SHARE = 0.75


def exchange(tiles, axis):
    return lax.all_to_all(tiles, axis, split_axis=0, concat_axis=0, tiled=True)


def from_everyone(x, axis):
    return exchange(jnp.broadcast_to(x, (lax.axis_size(axis), *x.shape)), axis)


def swapped(x, axis, flip):
    return lax.ppermute(x, axis, [(i, i ^ flip) for i in range(lax.axis_size(axis))])


def doubled(x, axis, flip):
    other = swapped(x, axis, flip)
    high = (lax.axis_index(axis) & flip) != 0
    return jnp.concatenate([jnp.where(high, other, x), jnp.where(high, x, other)], axis=0)


def tied(*values):
    return lax.optimization_barrier(values)


def summed(tiles):
    return tiles.astype(jnp.float32).sum(axis=0)


def forward_kernel(ids_ref, table_ref, proj_ref, emb_ref, normed_ref, inv_ref, even_ref, odd_ref, fm_ref):
    rank, n_emb = proj_ref.shape
    width = table_ref.shape[2]
    proj = proj_ref[...]
    for e in range(0, GROUP, 2):
        rows_ref = (even_ref, odd_ref)[e // 2 % 2]
        for r in range(2 * n_emb):
            rows_ref[pl.ds(r, 1), :] = table_ref[ids_ref[e + r // n_emb, r % n_emb]]
        pair = rows_ref[...].astype(jnp.bfloat16)
        first, second = pair[:n_emb], pair[n_emb:]
        emb_ref[e] = first
        emb_ref[e + 1] = second
        compressed = jnp.dot(
            proj, jnp.concatenate([first, second], axis=1), preferred_element_type=jnp.float32
        ).astype(jnp.bfloat16)
        compressed = jnp.concatenate([compressed[:, :width], compressed[:, width:]], axis=0)
        fm = lax.dot_general(compressed, pair, (((1,), (1,)), ((), ())), preferred_element_type=jnp.float32)
        fm_ref[pl.ds(e * rank, rank), :] = fm[:rank, :n_emb]
        fm_ref[pl.ds((e + 1) * rank, rank), :] = fm[rank:, n_emb:]
    scale = 1.0 / (rank * n_emb)
    parts = [fm_ref[pl.ds(k, GROUP, stride=rank), :] for k in range(rank)]
    mean = jnp.sum(sum(parts), axis=1, keepdims=True) * scale
    parts = [p - mean for p in parts]
    var = jnp.sum(sum(p * p for p in parts), axis=1, keepdims=True) * scale
    inv = 1.0 / jnp.sqrt(var + 1.0)
    per = normed_ref.shape[2] // n_emb
    for k in range(rank):
        at = k % per * n_emb
        normed_ref[k // per, :, at : at + n_emb] = (parts[k] * inv).astype(jnp.bfloat16)
    inv_ref[...] = jnp.broadcast_to(inv, inv_ref.shape)


def forward_features(ids, rows, projection, members, start, examples):
    n_emb = ids.shape[1]
    vocab, _, width = rows.shape
    rank = projection.shape[1]
    columns = rank * n_emb // members
    skip = start // GROUP
    return pl.pallas_call(
        forward_kernel,
        grid=(examples // GROUP,),
        in_specs=[
            pl.BlockSpec((GROUP, n_emb), lambda g: (g + skip, 0), memory_space=pltpu.SMEM),
            pl.BlockSpec((vocab, 1, width), lambda g: (0, 0, 0)),
            pl.BlockSpec((rank, n_emb), lambda g: (0, 0)),
        ],
        out_specs=[
            pl.BlockSpec((GROUP, n_emb, width), lambda g: (g, 0, 0)),
            pl.BlockSpec((members, GROUP, columns), lambda g: (0, g, 0)),
            pl.BlockSpec((GROUP, 128), lambda g: (g, 0)),
        ],
        out_shape=[
            jax.ShapeDtypeStruct((examples, n_emb, width), jnp.bfloat16),
            jax.ShapeDtypeStruct((members, examples, columns), jnp.bfloat16),
            jax.ShapeDtypeStruct((examples, 128), jnp.float32),
        ],
        scratch_shapes=[
            pltpu.VMEM((2 * n_emb, width), jnp.float32),
            pltpu.VMEM((2 * n_emb, width), jnp.float32),
            pltpu.VMEM((GROUP * rank, n_emb), jnp.float32),
        ],
        cost_estimate=pl.CostEstimate(
            flops=100_000_000 * examples,
            bytes_accessed=vocab * width * 4 + examples * n_emb * width * 2,
            transcendentals=0,
        ),
        name="fm_forward",
    )(ids, rows, projection.T)


def backward_kernel(grad_ref, normed_ref, inv_ref, emb_ref, back_ref, fm_grad_ref):
    n_emb = emb_ref.shape[1]
    rank, width = back_ref.shape[1:]
    per = normed_ref.shape[2] // n_emb
    scale = 1.0 / (rank * n_emb)
    grads = [grad_ref[:, k * n_emb : (k + 1) * n_emb] for k in range(rank)]
    normed = [
        normed_ref[k // per, :, k % per * n_emb : (k % per + 1) * n_emb].astype(jnp.float32) for k in range(rank)
    ]
    mean = jnp.sum(sum(grads), axis=1, keepdims=True) * scale
    along = jnp.sum(sum(g * x for g, x in zip(grads, normed)), axis=1, keepdims=True) * scale
    inv = inv_ref[:, :1]
    for k in range(rank):
        fm_grad_ref[pl.ds(k, GROUP, stride=rank), :] = (grads[k] - mean - normed[k] * along) * inv
    for e in range(0, GROUP, 2):
        fm_grad = fm_grad_ref[pl.ds(e * rank, 2 * rank), :].astype(jnp.bfloat16)
        pair = jnp.concatenate([emb_ref[e], emb_ref[e + 1]], axis=1)
        back = jnp.dot(fm_grad, pair, preferred_element_type=jnp.float32).astype(jnp.bfloat16)
        back_ref[e] = back[:rank, :width]
        back_ref[e + 1] = back[rank:, width:]


def backward_features(normed_grad, normed, inv_scale, embedded):
    examples, n_emb, width = embedded.shape
    members, _, columns = normed.shape
    rank = members * columns // n_emb
    return pl.pallas_call(
        backward_kernel,
        grid=(examples // GROUP,),
        in_specs=[
            pl.BlockSpec((GROUP, rank * n_emb), lambda g: (g, 0)),
            pl.BlockSpec((members, GROUP, columns), lambda g: (0, g, 0)),
            pl.BlockSpec((GROUP, 128), lambda g: (g, 0)),
            pl.BlockSpec((GROUP, n_emb, width), lambda g: (g, 0, 0)),
        ],
        out_specs=pl.BlockSpec((GROUP, rank, width), lambda g: (g, 0, 0)),
        out_shape=jax.ShapeDtypeStruct((examples, rank, width), jnp.bfloat16),
        scratch_shapes=[pltpu.VMEM((GROUP * rank, n_emb), jnp.float32)],
        cost_estimate=pl.CostEstimate(
            flops=30_000_000 * examples,
            bytes_accessed=examples * n_emb * (width * 2 + rank * 8),
            transcendentals=0,
        ),
        name="fm_backward",
    )(normed_grad, normed, inv_scale, embedded)


def both_halves(half):
    other = swapped(half, "c", 1)
    high = lax.axis_index("c") == 1
    return jnp.where(high, jnp.stack([other, half]), jnp.stack([half, other])).reshape(-1, *half.shape[1:])


def per_device(feature_ids, emb_table, factor_machine_projection, mlp_weight, momentum, hidden_grad, lcb_grad):
    mp, zl, y, x, c = (lax.axis_size(a) for a in ("mp", "zl", "y", "x", "c"))
    own = emb_table.shape[0]
    rank = factor_machine_projection.shape[1]
    examples, hidden = hidden_grad.shape

    to_worker = []
    for block in range(zl * y * x * c):
        cx, zy = divmod(block, zl * y)
        at_c, at_x = divmod(cx, x)
        to_worker.append((block, (zy * x + at_x) * c + at_c))
    to_owner = [(worker, owner) for owner, worker in to_worker]

    table = from_everyone(emb_table, ("mp", "zl", "y"))
    state = lax.ppermute(jnp.stack([mlp_weight, momentum]), DP, to_worker)
    weight_rows, momentum_rows = state[0], state[1]
    weights = weight_rows.astype(jnp.bfloat16)
    for axis, flip in (("y", 1), ("y", 2), ("y", 4), ("zl", 1)):
        weights = doubled(weights, axis, flip)
    table = from_everyone(table, "x").reshape(-1, emb_table.shape[1])
    weights, table = tied(weights, table)
    table = jnp.concatenate([table, swapped(table, "c", 1)], axis=0)
    rows = table.astype(jnp.float32).reshape(table.shape[0], 1, table.shape[1])
    weights = from_everyone(weights, "x").reshape(-1, hidden)
    owner, row = lax.div(feature_ids, own), lax.rem(feature_ids, own)
    owner, at_mp = lax.div(owner, mp), lax.rem(owner, mp)
    owner, at_c = lax.div(owner, c), lax.rem(owner, c)
    at_zy, at_x = lax.div(owner, x), lax.rem(owner, x)
    ids = ((((at_c ^ lax.axis_index("c")) * x + at_x) * mp + at_mp) * (zl * y) + at_zy) * own + row

    cut = int(examples * FIRST_SHARE)
    shares = ((0, cut), (cut, examples - cut))
    first = forward_features(ids, rows, factor_machine_projection, c * x, *shares[0])
    weights, ids, first_inv = tied(weights, ids, first[2])
    weights = both_halves(weights)
    second = forward_features(ids, rows, factor_machine_projection, c * x, *shares[1])
    features = ((first[0], first[1], first_inv), second)
    columns = [exchange(f[1], CX) for f in features]

    tiled_weights = weights.reshape(c * x, -1, hidden)
    preact = jnp.concatenate(
        [
            jnp.einsum("jbk,jkn->bn", normed, tiled_weights, preferred_element_type=jnp.float32)
            for _, normed, _ in features
        ],
        axis=0,
    )
    sigmoid_pre = jax.nn.sigmoid(preact)
    preact_grad = (
        hidden_grad.astype(jnp.float32) * sigmoid_pre * (1.0 + preact * (1.0 - sigmoid_pre))
    ).astype(jnp.bfloat16)
    group_grad = from_everyone(preact_grad, CX)

    proj_part, lcb_part = 0.0, 0.0
    for (embedded, normed, inv_scale), (start, count) in zip(features, shares):
        normed_part = lax.dot_general(
            preact_grad[start : start + count],
            weights,
            (((1,), (1,)), ((), ())),
            preferred_element_type=jnp.float32,
        )
        back = backward_features(normed_part, normed, inv_scale, embedded)
        proj_part += jnp.einsum("bqh,blh->ql", back, embedded, preferred_element_type=jnp.float32)
        lcb_part += jnp.einsum(
            "bld,bnd->ln", lcb_grad[start : start + count], embedded, preferred_element_type=jnp.float32
        )

    weight_grad = sum(
        lax.dot_general(
            part,
            group_grad[:, start : start + count],
            (((0, 1), (0, 1)), ((), ())),
            preferred_element_type=jnp.float32,
        )
        for part, (start, count) in zip(columns, shares)
    )
    weight_grad = exchange(weight_grad.astype(jnp.bfloat16).reshape(zl * y, -1, hidden), ZY)
    for flip in (1, 3):
        proj_part += swapped(proj_part, "mp", flip)
    both = jnp.concatenate([proj_part, lcb_part], axis=0)
    weight_grad, both = tied(weight_grad, both)
    new_momentum = 0.9 * momentum_rows + summed(weight_grad)
    new_weight = weight_rows - 0.01 * new_momentum
    next_weight = from_everyone(new_weight.astype(jnp.bfloat16), ZY)
    for axis, flip in (("c", 1), ("x", 1), ("x", 3)):
        both += swapped(both, axis, flip)
    next_weight, both = tied(next_weight, both)
    next_weight = from_everyone(next_weight, "x").reshape(-1, hidden)
    state = lax.ppermute(jnp.stack([new_weight, new_momentum]), DP, to_owner)
    for axis, flip in (("zl", 1), ("y", 1), ("y", 3)):
        both += swapped(both, axis, flip)
    next_weight, both, state = tied(next_weight, both, state)
    next_weight = both_halves(next_weight)
    both += swapped(both, "y", 7)
    return (state[0], state[1], next_weight, both[:rank].T, both[rank:].T)


def solution(mesh):
    torus = Mesh(mesh.devices.reshape(2, 8, 4, 2, mesh.shape["mp"]), DP_MP)
    placed = (
        P(DP, None),
        P(DP_MP, None),
        P(),
        P(DP, "mp"),
        P(DP, "mp"),
        P(DP, "mp"),
        P(DP, "mp", None),
    )

    return jax.shard_map(
        per_device,
        mesh=torus,
        in_specs=placed,
        out_specs=(P(DP, "mp"), P(DP, "mp"), P(None, "mp"), P(), P(None, "mp")),
        check_vma=False,
    )
```

```python
import jax
import jax.numpy as jnp
from jax import lax
from jax.experimental import pallas as pl
from jax.experimental.pallas import tpu as pltpu
from jax.sharding import Mesh
from jax.sharding import PartitionSpec as P


DP = ("zl", "y", "x", "c")
DP_MP = ("zl", "y", "x", "c", "mp")
CX = ("c", "x")
ZY = ("zl", "y")
GROUP = 32
ROWS = 8
FIRST_SHARE = 0.75


def exchange(tiles, axis):
    return lax.all_to_all(tiles, axis, split_axis=0, concat_axis=0, tiled=True)


def from_everyone(x, axis):
    return exchange(jnp.broadcast_to(x, (lax.axis_size(axis), *x.shape)), axis)


def swapped(x, axis, flip):
    return lax.ppermute(x, axis, [(i, i ^ flip) for i in range(lax.axis_size(axis))])


def over_four(x, axis):
    near, opposite, far = (
        lax.ppermute(x, axis, [(i, (i + step) % 4) for i in range(4)]) for step in (1, 2, 3)
    )
    return (x + opposite) + (near + far)


def in_parts(x):
    first = lax.reduce_precision(x, 8, 7)
    second = lax.reduce_precision(x - first, 8, 7)
    third = (x - first) - second
    top = jnp.concatenate([first, second], axis=-1)
    return jnp.concatenate([top, jnp.concatenate([third, jnp.zeros_like(third)], axis=-1)], axis=-2).astype(jnp.bfloat16)


def from_parts(parts):
    parts = parts.astype(jnp.float32)
    top, low = parts[..., :4, :], parts[..., 4:, :]
    return (top[..., :128] + top[..., 128:]) + low[..., :128]


def doubled(x, axis, flip):
    other = swapped(x, axis, flip)
    high = (lax.axis_index(axis) & flip) != 0
    return jnp.concatenate([jnp.where(high, other, x), jnp.where(high, x, other)], axis=0)


def tied(*values):
    return lax.optimization_barrier(values)


def summed(tiles):
    return tiles.astype(jnp.float32).sum(axis=0)


def forward_kernel(ids_ref, near_ref, far_ref, proj_ref, *refs):
    emb_ref, normed_ref, inv_ref, table_ref, even_ref, odd_ref, fm_ref = refs[-7:]
    rank, n_emb = proj_ref.shape
    half, width = near_ref.shape

    @pl.when(pl.program_id(0) == 0)
    def _():
        @pl.loop(0, half // 128)
        def _(i):
            at = pl.multiple_of(i * 128, 128)
            table_ref[pl.ds(at, 128), :] = near_ref[pl.ds(at, 128), :].astype(jnp.float32)
            table_ref[pl.ds(half + at, 128), :] = far_ref[pl.ds(at, 128), :].astype(jnp.float32)

    proj = proj_ref[...]
    scale = 1.0 / (rank * n_emb)
    per = normed_ref.shape[2] // n_emb
    for start in range(0, GROUP, ROWS):
        for e in range(0, ROWS, 2):
            rows_ref = (even_ref, odd_ref)[e // 2 % 2]
            for r in range(2 * n_emb):
                row = ids_ref[start + e + r // n_emb, r % n_emb]
                rows_ref[pl.ds(r, 1), :] = table_ref[pl.ds(row, 1), :]
            pair = rows_ref[...].astype(jnp.bfloat16)
            first, second = pair[:n_emb], pair[n_emb:]
            emb_ref[start + e] = first
            emb_ref[start + e + 1] = second
            compressed = jnp.dot(
                proj, jnp.concatenate([first, second], axis=1), preferred_element_type=jnp.float32
            ).astype(jnp.bfloat16)
            compressed = jnp.concatenate([compressed[:, :width], compressed[:, width:]], axis=0)
            fm = lax.dot_general(compressed, pair, (((1,), (1,)), ((), ())), preferred_element_type=jnp.float32)
            fm_ref[pl.ds(e * rank, rank), :] = fm[:rank, :n_emb]
            fm_ref[pl.ds((e + 1) * rank, rank), :] = fm[rank:, n_emb:]
        parts = [fm_ref[pl.ds(k, ROWS, stride=rank), :] for k in range(rank)]
        mean = jnp.sum(sum(parts), axis=1, keepdims=True) * scale
        parts = [p - mean for p in parts]
        var = jnp.sum(sum(p * p for p in parts), axis=1, keepdims=True) * scale
        inv = 1.0 / jnp.sqrt(var + 1.0)
        for k in range(rank):
            at = k % per * n_emb
            normed_ref[k // per, start : start + ROWS, at : at + n_emb] = (parts[k] * inv).astype(jnp.bfloat16)
        inv_ref[start : start + ROWS] = jnp.broadcast_to(inv, (ROWS, inv_ref.shape[1]))


def forward_features(ids, near, far, projection, blocks, start, count, embedded=None):
    examples, n_emb = ids.shape
    half, width = near.shape
    rank = projection.shape[1]
    columns = rank * n_emb // blocks
    skip = start // GROUP
    before = () if embedded is None else (embedded,)
    return pl.pallas_call(
        forward_kernel,
        grid=(count // GROUP,),
        in_specs=[
            pl.BlockSpec((GROUP, n_emb), lambda g: (g + skip, 0), memory_space=pltpu.SMEM),
            pl.BlockSpec((half, width), lambda g: (0, 0)),
            pl.BlockSpec((half, width), lambda g: (0, 0)),
            pl.BlockSpec((rank, n_emb), lambda g: (0, 0)),
            *(pl.BlockSpec(memory_space=pl.ANY) for _ in before),
        ],
        out_specs=[
            pl.BlockSpec((GROUP, n_emb, width), lambda g: (g + skip, 0, 0)),
            pl.BlockSpec((blocks, GROUP, columns), lambda g: (0, g, 0)),
            pl.BlockSpec((GROUP, 128), lambda g: (g, 0)),
        ],
        out_shape=[
            jax.ShapeDtypeStruct((examples, n_emb, width), jnp.bfloat16),
            jax.ShapeDtypeStruct((blocks, count, columns), jnp.bfloat16),
            jax.ShapeDtypeStruct((count, 128), jnp.float32),
        ],
        scratch_shapes=[
            pltpu.VMEM((2 * half, width), jnp.float32),
            pltpu.VMEM((2 * n_emb, width), jnp.float32),
            pltpu.VMEM((2 * n_emb, width), jnp.float32),
            pltpu.VMEM((ROWS * rank, n_emb), jnp.float32),
        ],
        input_output_aliases={4: 0} if before else {},
        cost_estimate=pl.CostEstimate(
            flops=100_000_000 * count,
            bytes_accessed=half * width * 4 + count * n_emb * width * 2,
            transcendentals=0,
        ),
        name="fm_forward",
    )(ids, near, far, projection.T, *before)


def backward_kernel(grad_ref, normed_ref, inv_ref, emb_ref, *refs):
    back_ref, fm_grad_ref = refs[-2:]
    n_emb = emb_ref.shape[1]
    rank, width = back_ref.shape[1:]
    per = normed_ref.shape[2] // n_emb
    scale = 1.0 / (rank * n_emb)
    for start in range(0, GROUP, ROWS):
        rows = slice(start, start + ROWS)
        grads = [grad_ref[rows, k * n_emb : (k + 1) * n_emb] for k in range(rank)]
        normed = [
            normed_ref[k // per, rows, k % per * n_emb : (k % per + 1) * n_emb].astype(jnp.float32)
            for k in range(rank)
        ]
        mean = jnp.sum(sum(grads), axis=1, keepdims=True) * scale
        along = jnp.sum(sum(g * x for g, x in zip(grads, normed)), axis=1, keepdims=True) * scale
        inv = inv_ref[rows, :1]
        for k in range(rank):
            fm_grad_ref[pl.ds(k, ROWS, stride=rank), :] = (grads[k] - mean - normed[k] * along) * inv
        for e in range(0, ROWS, 2):
            fm_grad = fm_grad_ref[pl.ds(e * rank, 2 * rank), :].astype(jnp.bfloat16)
            pair = jnp.concatenate([emb_ref[start + e], emb_ref[start + e + 1]], axis=1)
            back = jnp.dot(fm_grad, pair, preferred_element_type=jnp.float32).astype(jnp.bfloat16)
            back_ref[start + e] = back[:rank, :width]
            back_ref[start + e + 1] = back[rank:, width:]


def backward_features(normed_grad, normed, inv_scale, embedded, start, back=None):
    examples, n_emb, width = embedded.shape
    blocks, count, columns = normed.shape
    rank = blocks * columns // n_emb
    skip = start // GROUP
    before = () if back is None else (back,)
    return pl.pallas_call(
        backward_kernel,
        grid=(count // GROUP,),
        in_specs=[
            pl.BlockSpec((GROUP, rank * n_emb), lambda g: (g + skip, 0)),
            pl.BlockSpec((blocks, GROUP, columns), lambda g: (0, g, 0)),
            pl.BlockSpec((GROUP, 128), lambda g: (g, 0)),
            pl.BlockSpec((GROUP, n_emb, width), lambda g: (g + skip, 0, 0)),
            *(pl.BlockSpec(memory_space=pl.ANY) for _ in before),
        ],
        out_specs=pl.BlockSpec((GROUP, rank, width), lambda g: (g + skip, 0, 0)),
        out_shape=jax.ShapeDtypeStruct((examples, rank, width), jnp.bfloat16),
        scratch_shapes=[pltpu.VMEM((ROWS * rank, n_emb), jnp.float32)],
        input_output_aliases={4: 0} if before else {},
        cost_estimate=pl.CostEstimate(
            flops=30_000_000 * count,
            bytes_accessed=count * n_emb * (width * 2 + rank * 8),
            transcendentals=0,
        ),
        name="fm_backward",
    )(normed_grad, normed, inv_scale, embedded, *before)


def both_halves(half):
    other = swapped(half, "c", 1)
    high = lax.axis_index("c") == 1
    return jnp.where(high, jnp.stack([other, half]), jnp.stack([half, other])).reshape(-1, *half.shape[1:])


def per_device(feature_ids, emb_table, factor_machine_projection, mlp_weight, momentum, hidden_grad, lcb_grad):
    mp, zl, y, x, c = (lax.axis_size(a) for a in ("mp", "zl", "y", "x", "c"))
    own = emb_table.shape[0]
    rank = factor_machine_projection.shape[1]
    examples, hidden = hidden_grad.shape

    to_worker = []
    for block in range(zl * y * x * c):
        cx, zy = divmod(block, zl * y)
        at_c, at_x = divmod(cx, x)
        to_worker.append((block, (zy * x + at_x) * c + at_c))
    to_owner = [(worker, owner) for owner, worker in to_worker]

    width = emb_table.shape[1]
    table = from_everyone(emb_table, ("mp", "zl")).reshape(-1, width)
    state = lax.ppermute(jnp.stack([mlp_weight, momentum]), DP, to_worker)
    weight_rows, momentum_rows = state[0], state[1]
    weights = weight_rows.astype(jnp.bfloat16)
    near_rows = table.shape[0]
    table = from_everyone(jnp.concatenate([table, weights[:, :width], weights[:, width:]], axis=0), "y")
    weights = table[:, near_rows:].reshape(y, hidden // width, -1, width)
    weights = jnp.swapaxes(weights, 1, 2).reshape(-1, hidden)
    weights = doubled(weights, "zl", 1)
    table = from_everyone(table[:, :near_rows], "x").reshape(-1, width)
    weights, table = tied(weights, table)
    table_far = swapped(table, "c", 1)
    weights = from_everyone(weights, "x").reshape(-1, hidden)
    owner, row = lax.div(feature_ids, own), lax.rem(feature_ids, own)
    owner, at_mp = lax.div(owner, mp), lax.rem(owner, mp)
    owner, at_c = lax.div(owner, c), lax.rem(owner, c)
    owner, at_x = lax.div(owner, x), lax.rem(owner, x)
    at_zl, at_y = lax.div(owner, y), lax.rem(owner, y)
    ids = (((((at_c ^ lax.axis_index("c")) * x + at_x) * y + at_y) * mp + at_mp) * zl + at_zl) * own + row

    blocks = 2 * c * x
    cut = int(examples * FIRST_SHARE)
    shares = ((0, cut), (cut, examples - cut))
    embedded, normed_a, inv_a = forward_features(ids, table, table_far, factor_machine_projection, blocks, *shares[0])
    weights = both_halves(weights)
    embedded, normed_b, inv_b = forward_features(
        ids, table, table_far, factor_machine_projection, blocks, *shares[1], embedded
    )
    columns_a = exchange(normed_a.reshape(c * x, 2 * cut, -1), CX)

    tiled_weights = weights.reshape(blocks, -1, hidden)
    preact = jnp.concatenate(
        [
            jnp.einsum("jbk,jkn->bn", normed, tiled_weights, preferred_element_type=jnp.float32)
            for normed in (normed_a, normed_b)
        ],
        axis=0,
    )
    sigmoid_pre = jax.nn.sigmoid(preact)
    preact_grad = (
        hidden_grad.astype(jnp.float32) * sigmoid_pre * (1.0 + preact * (1.0 - sigmoid_pre))
    ).astype(jnp.bfloat16)
    group_grad = exchange(
        jnp.concatenate(
            [
                jnp.broadcast_to(preact_grad, (c * x, examples, hidden)),
                normed_b.reshape(c * x, -1, hidden),
            ],
            axis=1,
        ),
        CX,
    )

    normed_part = lax.dot_general(preact_grad, weights, (((1,), (1,)), ((), ())), preferred_element_type=jnp.float32)
    back = backward_features(normed_part, normed_a, inv_a, embedded, 0)
    back = backward_features(normed_part, normed_b, inv_b, embedded, cut, back)
    proj_part = jnp.einsum("bqh,blh->ql", back, embedded, preferred_element_type=jnp.float32)
    lcb_part = jnp.einsum("bld,bnd->ln", lcb_grad, embedded, preferred_element_type=jnp.float32)
    both = jnp.concatenate([proj_part, lcb_part], axis=0)

    weight_grad = 0.0
    columns_b = group_grad[:, examples:]
    for part, (start, count) in zip((columns_a, columns_b), shares):
        weight_grad += jnp.einsum(
            "shbk,sbn->hkn",
            part.reshape(c * x, 2, count, -1),
            group_grad[:, start : start + count],
            preferred_element_type=jnp.float32,
        )
    arrived = exchange(
        jnp.concatenate(
            [
                weight_grad.astype(jnp.bfloat16).reshape(zl * y, -1, hidden),
                in_parts(both.reshape(zl * y, -1, both.shape[1])),
            ],
            axis=1,
        ),
        ZY,
    )
    own_rows = weight_rows.shape[0]
    both = from_parts(summed(arrived[:, own_rows:]))
    new_momentum = 0.9 * momentum_rows + summed(arrived[:, :own_rows])
    new_weight = weight_rows - 0.01 * new_momentum
    arrived = from_everyone(jnp.concatenate([new_weight.astype(jnp.bfloat16), in_parts(both)], axis=0), ZY)
    next_weight = from_everyone(arrived[:, :own_rows], "x").reshape(-1, hidden)
    both = from_parts(arrived[:, own_rows:]).reshape(-1, both.shape[1])
    state = lax.ppermute(jnp.stack([new_weight, new_momentum]), DP, to_owner)
    proj_sum = over_four(both[:rank], "mp")
    both = over_four(jnp.concatenate([proj_sum, both[rank:]], axis=0), "x")
    next_weight, both, state = tied(next_weight, both, state)
    next_weight = both_halves(next_weight)
    both += swapped(both, "c", 1)
    return (state[0], state[1], next_weight, both[:rank].T, both[rank:].T)


def solution(mesh):
    torus = Mesh(mesh.devices.reshape(2, 8, 4, 2, mesh.shape["mp"]), DP_MP)
    placed = (
        P(DP, None),
        P(DP_MP, None),
        P(),
        P(DP, "mp"),
        P(DP, "mp"),
        P(DP, "mp"),
        P(DP, "mp", None),
    )

    return jax.shard_map(
        per_device,
        mesh=torus,
        in_specs=placed,
        out_specs=(P(DP, "mp"), P(DP, "mp"), P(None, "mp"), P(), P(None, "mp")),
        check_vma=False,
    )
```

```python
import jax
import jax.numpy as jnp
from jax import lax
from jax.experimental import pallas as pl
from jax.experimental.pallas import tpu as pltpu
from jax.sharding import Mesh
from jax.sharding import PartitionSpec as P


DP = ("zl", "y", "x", "c")
DP_MP = ("zl", "y", "x", "c", "mp")
CX = ("c", "x")
ZY = ("zl", "y")
GROUP = 32
ROWS = 8
FIRST_SHARE = 0.75


def exchange(tiles, axis):
    return lax.all_to_all(tiles, axis, split_axis=0, concat_axis=0, tiled=True)


def from_everyone(x, axis):
    return exchange(jnp.broadcast_to(x, (lax.axis_size(axis), *x.shape)), axis)


def swapped(x, axis, flip):
    return lax.ppermute(x, axis, [(i, i ^ flip) for i in range(lax.axis_size(axis))])


def in_parts(x):
    first = lax.reduce_precision(x, 8, 7)
    second = lax.reduce_precision(x - first, 8, 7)
    third = (x - first) - second
    top = jnp.concatenate([first, second], axis=-1)
    return jnp.concatenate([top, jnp.concatenate([third, jnp.zeros_like(third)], axis=-1)], axis=-2).astype(jnp.bfloat16)


def from_parts(parts):
    parts = parts.astype(jnp.float32)
    top, low = parts[..., :4, :], parts[..., 4:, :]
    return (top[..., :128] + top[..., 128:]) + low[..., :128]


def doubled(x, axis, flip):
    other = swapped(x, axis, flip)
    high = (lax.axis_index(axis) & flip) != 0
    return jnp.concatenate([jnp.where(high, other, x), jnp.where(high, x, other)], axis=0)


def tied(*values):
    return lax.optimization_barrier(values)


def summed(tiles):
    return tiles.astype(jnp.float32).sum(axis=0)


def forward_kernel(ids_ref, near_ref, far_ref, proj_ref, lcb_ref, *refs):
    emb_ref, normed_ref, inv_ref, lcb_sum_ref, table_ref, even_ref, odd_ref, fm_ref = refs[-8:]
    rank, n_emb = proj_ref.shape
    half, width = near_ref.shape

    @pl.when(pl.program_id(0) == 0)
    def _():
        lcb_sum_ref[...] = jnp.zeros_like(lcb_sum_ref)

        @pl.loop(0, half // 128)
        def _(i):
            at = pl.multiple_of(i * 128, 128)
            table_ref[pl.ds(at, 128), :] = near_ref[pl.ds(at, 128), :].astype(jnp.float32)
            table_ref[pl.ds(half + at, 128), :] = far_ref[pl.ds(at, 128), :].astype(jnp.float32)

    proj = proj_ref[...]
    scale = 1.0 / (rank * n_emb)
    per = normed_ref.shape[2] // n_emb
    outputs = lcb_ref.shape[1]
    lcb_sum = jnp.zeros(lcb_sum_ref.shape, jnp.float32)
    for start in range(0, GROUP, ROWS):
        for e in range(0, ROWS, 2):
            rows_ref = (even_ref, odd_ref)[e // 2 % 2]
            for r in range(2 * n_emb):
                row = ids_ref[start + e + r // n_emb, r % n_emb]
                rows_ref[pl.ds(r, 1), :] = table_ref[pl.ds(row, 1), :]
            pair = rows_ref[...].astype(jnp.bfloat16)
            first, second = pair[:n_emb], pair[n_emb:]
            emb_ref[start + e] = first
            emb_ref[start + e + 1] = second
            compressed = jnp.dot(
                proj, jnp.concatenate([first, second], axis=1), preferred_element_type=jnp.float32
            ).astype(jnp.bfloat16)
            left = jnp.concatenate(
                [compressed[:, :width], compressed[:, width:], lcb_ref[start + e], lcb_ref[start + e + 1]], axis=0
            )
            fm = lax.dot_general(left, pair, (((1,), (1,)), ((), ())), preferred_element_type=jnp.float32)
            fm_ref[pl.ds(e * rank, rank), :] = fm[:rank, :n_emb]
            fm_ref[pl.ds((e + 1) * rank, rank), :] = fm[rank : 2 * rank, n_emb:]
            lcb_sum += fm[2 * rank : 2 * rank + outputs, :n_emb] + fm[2 * rank + outputs :, n_emb:]
        parts = [fm_ref[pl.ds(k, ROWS, stride=rank), :] for k in range(rank)]
        mean = jnp.sum(sum(parts), axis=1, keepdims=True) * scale
        parts = [p - mean for p in parts]
        var = jnp.sum(sum(p * p for p in parts), axis=1, keepdims=True) * scale
        inv = 1.0 / jnp.sqrt(var + 1.0)
        for k in range(rank):
            at = k % per * n_emb
            normed_ref[k // per, start : start + ROWS, at : at + n_emb] = (parts[k] * inv).astype(jnp.bfloat16)
        inv_ref[start : start + ROWS] = jnp.broadcast_to(inv, (ROWS, inv_ref.shape[1]))
    lcb_sum_ref[...] += lcb_sum


def forward_features(ids, near, far, projection, lcb_grad, blocks, start, count, before=()):
    examples, n_emb = ids.shape
    half, width = near.shape
    rank = projection.shape[1]
    columns = rank * n_emb // blocks
    skip = start // GROUP
    outputs = lcb_grad.shape[1]
    return pl.pallas_call(
        forward_kernel,
        grid=(count // GROUP,),
        in_specs=[
            pl.BlockSpec((GROUP, n_emb), lambda g: (g + skip, 0), memory_space=pltpu.SMEM),
            pl.BlockSpec((half, width), lambda g: (0, 0)),
            pl.BlockSpec((half, width), lambda g: (0, 0)),
            pl.BlockSpec((rank, n_emb), lambda g: (0, 0)),
            pl.BlockSpec((GROUP, outputs, width), lambda g: (g + skip, 0, 0)),
            *(pl.BlockSpec(memory_space=pl.ANY) for _ in before),
        ],
        out_specs=[
            pl.BlockSpec((GROUP, n_emb, width), lambda g: (g + skip, 0, 0)),
            pl.BlockSpec((blocks, GROUP, columns), lambda g: (0, g, 0)),
            pl.BlockSpec((GROUP, 128), lambda g: (g + skip, 0)),
            pl.BlockSpec((outputs, n_emb), lambda g: (0, 0)),
        ],
        out_shape=[
            jax.ShapeDtypeStruct((examples, n_emb, width), jnp.bfloat16),
            jax.ShapeDtypeStruct((blocks, count, columns), jnp.bfloat16),
            jax.ShapeDtypeStruct((examples, 128), jnp.float32),
            jax.ShapeDtypeStruct((outputs, n_emb), jnp.float32),
        ],
        scratch_shapes=[
            pltpu.VMEM((2 * half, width), jnp.float32),
            pltpu.VMEM((2 * n_emb, width), jnp.float32),
            pltpu.VMEM((2 * n_emb, width), jnp.float32),
            pltpu.VMEM((ROWS * rank, n_emb), jnp.float32),
        ],
        input_output_aliases={5: 0, 6: 2} if before else {},
        cost_estimate=pl.CostEstimate(
            flops=100_000_000 * count,
            bytes_accessed=half * width * 4 + count * n_emb * width * 2,
            transcendentals=0,
        ),
        name="fm_forward",
    )(ids, near, far, projection.T, lcb_grad, *before)


def backward_kernel(grad_ref, first_ref, last_ref, inv_ref, emb_ref, proj_ref, fm_grad_ref):
    n_emb, rank = proj_ref.shape
    width = emb_ref.shape[2]
    per = last_ref.shape[2] // n_emb
    scale = 1.0 / (rank * n_emb)
    at_last = pl.program_id(0) == pl.num_programs(0) - 1

    @pl.when(pl.program_id(0) == 0)
    def _():
        proj_ref[...] = jnp.zeros_like(proj_ref)

    proj = jnp.zeros(proj_ref.shape, jnp.float32)
    for start in range(0, GROUP, ROWS):
        rows = slice(start, start + ROWS)
        grads = [grad_ref[rows, k * n_emb : (k + 1) * n_emb] for k in range(rank)]
        cuts = [(k // per, rows, slice(k % per * n_emb, (k % per + 1) * n_emb)) for k in range(rank)]
        normed = [
            jnp.where(at_last, last_ref[cut].astype(jnp.float32), first_ref[cut].astype(jnp.float32)) for cut in cuts
        ]
        mean = jnp.sum(sum(grads), axis=1, keepdims=True) * scale
        along = jnp.sum(sum(g * x for g, x in zip(grads, normed)), axis=1, keepdims=True) * scale
        inv = inv_ref[rows, :1]
        for k in range(rank):
            fm_grad_ref[pl.ds(k, ROWS, stride=rank), :] = (grads[k] - mean - normed[k] * along) * inv
        for e in range(0, ROWS, 2):
            fm_grad = fm_grad_ref[pl.ds(e * rank, 2 * rank), :].astype(jnp.bfloat16)
            pair = jnp.concatenate([emb_ref[start + e], emb_ref[start + e + 1]], axis=1)
            back = jnp.dot(fm_grad, pair, preferred_element_type=jnp.float32).astype(jnp.bfloat16)
            back = jnp.concatenate([back[:rank, :width], back[rank:, width:]], axis=1)
            proj += lax.dot_general(pair, back, (((1,), (1,)), ((), ())), preferred_element_type=jnp.float32)
    proj_ref[...] += proj


def backward_features(normed_grad, normed_first, normed_last, inv_scale, embedded):
    examples, n_emb, width = embedded.shape
    blocks, count, columns = normed_first.shape
    rank = blocks * columns // n_emb
    firsts = count // GROUP
    assert normed_last.shape[1] == GROUP and count + GROUP == examples
    return pl.pallas_call(
        backward_kernel,
        grid=(firsts + 1,),
        in_specs=[
            pl.BlockSpec((GROUP, rank * n_emb), lambda g: (g, 0)),
            pl.BlockSpec((blocks, GROUP, columns), lambda g: (0, jnp.minimum(g, firsts - 1), 0)),
            pl.BlockSpec((blocks, GROUP, columns), lambda g: (0, 0, 0)),
            pl.BlockSpec((GROUP, 128), lambda g: (g, 0)),
            pl.BlockSpec((GROUP, n_emb, width), lambda g: (g, 0, 0)),
        ],
        out_specs=pl.BlockSpec((n_emb, rank), lambda g: (0, 0)),
        out_shape=jax.ShapeDtypeStruct((n_emb, rank), jnp.float32),
        scratch_shapes=[pltpu.VMEM((ROWS * rank, n_emb), jnp.float32)],
        cost_estimate=pl.CostEstimate(
            flops=40_000_000 * examples,
            bytes_accessed=examples * n_emb * (width * 2 + rank * 6),
            transcendentals=0,
        ),
        name="fm_backward",
    )(normed_grad, normed_first, normed_last, inv_scale, embedded)


def both_halves(half, order=None):
    other = swapped(half, "c", 1)
    high = lax.axis_index("c") == 1
    if order is None:
        return jnp.where(high, jnp.stack([other, half]), jnp.stack([half, other])).reshape(-1, *half.shape[1:])
    dims, axes = order
    both = [h.reshape(*dims, *half.shape[1:]) for h in (half, other)]
    both = jnp.where(high, jnp.stack(both[::-1]), jnp.stack(both))
    return jnp.transpose(both, axes).reshape(-1, *half.shape[1:])


def per_device(feature_ids, emb_table, factor_machine_projection, mlp_weight, momentum, hidden_grad, lcb_grad):
    mp, zl, y, x, c = (lax.axis_size(a) for a in ("mp", "zl", "y", "x", "c"))
    own = emb_table.shape[0]
    rank = factor_machine_projection.shape[1]
    examples, hidden = hidden_grad.shape

    to_worker = []
    for block in range(zl * y * x * c):
        cx, zy = divmod(block, zl * y)
        at_c, at_x = divmod(cx, x)
        to_worker.append((block, (zy * x + at_x) * c + at_c))
    to_owner = [(worker, owner) for owner, worker in to_worker]

    width = emb_table.shape[1]
    table = from_everyone(emb_table, ("mp", "zl")).reshape(-1, width)
    state = lax.ppermute(jnp.stack([mlp_weight, momentum]), DP, to_worker)
    weight_rows, momentum_rows = state[0], state[1]
    weights = mlp_weight.astype(jnp.bfloat16)
    near_rows = table.shape[0]
    table = from_everyone(jnp.concatenate([table, weights[:, :width], weights[:, width:]], axis=0), "y")
    weights = table[:, near_rows:].reshape(y, hidden // width, -1, width)
    weights = jnp.swapaxes(weights, 1, 2).reshape(-1, hidden)
    weights = doubled(weights, "zl", 1)
    table = from_everyone(table[:, :near_rows], "x").reshape(-1, width)
    weights, table = tied(weights, table)
    table_far = swapped(table, "c", 1)
    weights = from_everyone(weights, "x").reshape(-1, hidden)
    owner, row = lax.div(feature_ids, own), lax.rem(feature_ids, own)
    owner, at_mp = lax.div(owner, mp), lax.rem(owner, mp)
    owner, at_c = lax.div(owner, c), lax.rem(owner, c)
    owner, at_x = lax.div(owner, x), lax.rem(owner, x)
    at_zl, at_y = lax.div(owner, y), lax.rem(owner, y)
    ids = (((((at_c ^ lax.axis_index("c")) * x + at_x) * y + at_y) * mp + at_mp) * zl + at_zl) * own + row

    blocks = 2 * c * x
    cut = int(examples * FIRST_SHARE)
    shares = ((0, cut), (cut, examples - cut))
    inputs = (ids, table, table_far, factor_machine_projection, lcb_grad)
    embedded, normed_a, inv_scale, lcb_a = forward_features(*inputs, blocks, *shares[0])
    weights = both_halves(weights, ((x, zl, y, mlp_weight.shape[0]), (2, 3, 1, 0, 4, 5)))
    embedded, normed_b, inv_scale, lcb_b = forward_features(
        *inputs, blocks, *shares[1], (embedded, inv_scale)
    )
    columns_a = exchange(normed_a.reshape(c * x, 2 * cut, -1), CX)

    tiled_weights = weights.reshape(blocks, -1, hidden)
    preact = jnp.concatenate(
        [
            jnp.einsum("jbk,jkn->bn", normed, tiled_weights, preferred_element_type=jnp.float32)
            for normed in (normed_a, normed_b)
        ],
        axis=0,
    )
    sigmoid_pre = jax.nn.sigmoid(preact)
    preact_grad = (
        hidden_grad.astype(jnp.float32) * sigmoid_pre * (1.0 + preact * (1.0 - sigmoid_pre))
    ).astype(jnp.bfloat16)
    group_grad = exchange(
        jnp.concatenate(
            [
                jnp.broadcast_to(preact_grad, (c * x, examples, hidden)),
                normed_b.reshape(c * x, -1, hidden),
            ],
            axis=1,
        ),
        CX,
    )

    normed_part = lax.dot_general(preact_grad, weights, (((1,), (1,)), ((), ())), preferred_element_type=jnp.float32)
    proj_part = backward_features(normed_part, normed_a, normed_b, inv_scale, embedded)
    both = jnp.concatenate([proj_part.T, lcb_a + lcb_b], axis=0)

    (start_a, count_a), (start_b, count_b) = shares
    weight_grad = jnp.einsum(
        "shbk,sbn->hkn",
        columns_a.reshape(c * x, 2, count_a, -1),
        group_grad[:, :count_a],
        preferred_element_type=jnp.float32,
    ) + jnp.stack(
        [
            jnp.einsum(
                "sbk,sbn->kn",
                group_grad[:, at : at + count_b],
                group_grad[:, start_b:examples],
                preferred_element_type=jnp.float32,
            )
            for at in (examples, examples + count_b)
        ]
    )
    arrived = exchange(
        jnp.concatenate(
            [
                weight_grad.astype(jnp.bfloat16).reshape(zl * y, -1, hidden),
                in_parts(both.reshape(zl * y, -1, both.shape[1])),
            ],
            axis=1,
        ),
        ZY,
    )
    own_rows = weight_rows.shape[0]
    both = from_parts(summed(arrived[:, own_rows:]))
    new_momentum = 0.9 * momentum_rows + summed(arrived[:, :own_rows])
    new_weight = weight_rows - 0.01 * new_momentum
    next_weight = from_everyone(new_weight.astype(jnp.bfloat16), ZY)
    over_mp = both + swapped(both, "mp", 1)
    over_mp += swapped(over_mp, "mp", 3)
    both = jnp.where(lax.axis_index("zl") == 0, over_mp, both)
    both += swapped(both, "c", 1)
    next_weight, both = tied(next_weight, both)
    next_weight = from_everyone(next_weight, "x").reshape(-1, hidden)
    state = lax.ppermute(jnp.stack([new_weight, new_momentum]), DP, to_owner)
    both += swapped(both, "x", 1)
    both += swapped(both, "x", 3)
    next_weight, both, state = tied(next_weight, both, state)
    next_weight = both_halves(next_weight)
    both = from_everyone(both, ZY).reshape(2 * rank, -1)
    return (state[0], state[1], next_weight, both[:rank].T, both[rank:].T)


def solution(mesh):
    torus = Mesh(mesh.devices.reshape(2, 8, 4, 2, mesh.shape["mp"]), DP_MP)
    placed = (
        P(DP, None),
        P(DP_MP, None),
        P(),
        P(DP, "mp"),
        P(DP, "mp"),
        P(DP, "mp"),
        P(DP, "mp", None),
    )

    return jax.shard_map(
        per_device,
        mesh=torus,
        in_specs=placed,
        out_specs=(P(DP, "mp"), P(DP, "mp"), P(None, "mp"), P(), P(None, "mp")),
        check_vma=False,
    )
```

```python
import jax
import jax.numpy as jnp
from jax import lax
from jax.experimental import pallas as pl
from jax.experimental.pallas import tpu as pltpu
from jax.sharding import Mesh
from jax.sharding import PartitionSpec as P


DP = ("zl", "y", "x", "c")
DP_MP = ("zl", "y", "x", "c", "mp")
CX = ("c", "x")
ZY = ("zl", "y")
GROUP = 32
ROWS = 8
FIRST_SHARE = 0.75


def exchange(tiles, axis):
    return lax.all_to_all(tiles, axis, split_axis=0, concat_axis=0, tiled=True)


def from_everyone(x, axis):
    return exchange(jnp.broadcast_to(x, (lax.axis_size(axis), *x.shape)), axis)


def swapped(x, axis, flip):
    return lax.ppermute(x, axis, [(i, i ^ flip) for i in range(lax.axis_size(axis))])


def in_two_parts(x):
    first = lax.reduce_precision(x, 8, 7)
    return jnp.concatenate([first, x - first], axis=0).astype(jnp.bfloat16)


def doubled(x, axis, flip):
    other = swapped(x, axis, flip)
    high = (lax.axis_index(axis) & flip) != 0
    return jnp.concatenate([jnp.where(high, other, x), jnp.where(high, x, other)], axis=0)


def tied(*values):
    return lax.optimization_barrier(values)


def summed(tiles):
    return tiles.astype(jnp.float32).sum(axis=0)


def forward_kernel(ids_ref, near_ref, far_ref, proj_ref, lcb_ref, *refs):
    emb_ref, normed_ref, inv_ref, lcb_sum_ref, table_ref, even_ref, odd_ref, fm_ref = refs[-8:]
    rank, n_emb = proj_ref.shape
    half, width = near_ref.shape

    @pl.when(pl.program_id(0) == 0)
    def _():
        lcb_sum_ref[...] = jnp.zeros_like(lcb_sum_ref)

        @pl.loop(0, half // 128)
        def _(i):
            at = pl.multiple_of(i * 128, 128)
            table_ref[pl.ds(at, 128), :] = near_ref[pl.ds(at, 128), :].astype(jnp.float32)
            table_ref[pl.ds(half + at, 128), :] = far_ref[pl.ds(at, 128), :].astype(jnp.float32)

    proj = proj_ref[...]
    scale = 1.0 / (rank * n_emb)
    per = normed_ref.shape[2] // n_emb
    outputs = lcb_ref.shape[1]
    lcb_sum = jnp.zeros(lcb_sum_ref.shape, jnp.float32)
    for start in range(0, GROUP, ROWS):
        for e in range(0, ROWS, 2):
            rows_ref = (even_ref, odd_ref)[e // 2 % 2]
            for r in range(2 * n_emb):
                row = ids_ref[start + e + r // n_emb, r % n_emb]
                rows_ref[pl.ds(r, 1), :] = table_ref[pl.ds(row, 1), :]
            pair = rows_ref[...].astype(jnp.bfloat16)
            first, second = pair[:n_emb], pair[n_emb:]
            emb_ref[start + e] = first
            emb_ref[start + e + 1] = second
            compressed = jnp.dot(
                proj, jnp.concatenate([first, second], axis=1), preferred_element_type=jnp.float32
            ).astype(jnp.bfloat16)
            left = jnp.concatenate(
                [compressed[:, :width], compressed[:, width:], lcb_ref[start + e], lcb_ref[start + e + 1]], axis=0
            )
            fm = lax.dot_general(left, pair, (((1,), (1,)), ((), ())), preferred_element_type=jnp.float32)
            fm_ref[pl.ds(e * rank, rank), :] = fm[:rank, :n_emb]
            fm_ref[pl.ds((e + 1) * rank, rank), :] = fm[rank : 2 * rank, n_emb:]
            lcb_sum += fm[2 * rank : 2 * rank + outputs, :n_emb] + fm[2 * rank + outputs :, n_emb:]
        parts = [fm_ref[pl.ds(k, ROWS, stride=rank), :] for k in range(rank)]
        mean = jnp.sum(sum(parts), axis=1, keepdims=True) * scale
        parts = [p - mean for p in parts]
        var = jnp.sum(sum(p * p for p in parts), axis=1, keepdims=True) * scale
        inv = 1.0 / jnp.sqrt(var + 1.0)
        for k in range(rank):
            at = k % per * n_emb
            normed_ref[k // per, start : start + ROWS, at : at + n_emb] = (parts[k] * inv).astype(jnp.bfloat16)
        inv_ref[start : start + ROWS] = jnp.broadcast_to(inv, (ROWS, inv_ref.shape[1]))
    lcb_sum_ref[...] += lcb_sum


def forward_features(ids, near, far, projection, lcb_grad, blocks, start, count, before=()):
    examples, n_emb = ids.shape
    half, width = near.shape
    rank = projection.shape[1]
    columns = rank * n_emb // blocks
    skip = start // GROUP
    outputs = lcb_grad.shape[1]
    return pl.pallas_call(
        forward_kernel,
        grid=(count // GROUP,),
        in_specs=[
            pl.BlockSpec((GROUP, n_emb), lambda g: (g + skip, 0), memory_space=pltpu.SMEM),
            pl.BlockSpec((half, width), lambda g: (0, 0)),
            pl.BlockSpec((half, width), lambda g: (0, 0)),
            pl.BlockSpec((rank, n_emb), lambda g: (0, 0)),
            pl.BlockSpec((GROUP, outputs, width), lambda g: (g + skip, 0, 0)),
            *(pl.BlockSpec(memory_space=pl.ANY) for _ in before),
        ],
        out_specs=[
            pl.BlockSpec((GROUP, n_emb, width), lambda g: (g + skip, 0, 0)),
            pl.BlockSpec((blocks, GROUP, columns), lambda g: (0, g, 0)),
            pl.BlockSpec((GROUP, 128), lambda g: (g + skip, 0)),
            pl.BlockSpec((outputs, n_emb), lambda g: (0, 0)),
        ],
        out_shape=[
            jax.ShapeDtypeStruct((examples, n_emb, width), jnp.bfloat16),
            jax.ShapeDtypeStruct((blocks, count, columns), jnp.bfloat16),
            jax.ShapeDtypeStruct((examples, 128), jnp.float32),
            jax.ShapeDtypeStruct((outputs, n_emb), jnp.float32),
        ],
        scratch_shapes=[
            pltpu.VMEM((2 * half, width), jnp.float32),
            pltpu.VMEM((2 * n_emb, width), jnp.float32),
            pltpu.VMEM((2 * n_emb, width), jnp.float32),
            pltpu.VMEM((ROWS * rank, n_emb), jnp.float32),
        ],
        input_output_aliases={5: 0, 6: 2} if before else {},
        cost_estimate=pl.CostEstimate(
            flops=100_000_000 * count,
            bytes_accessed=half * width * 4 + count * n_emb * width * 2,
            transcendentals=0,
        ),
        name="fm_forward",
    )(ids, near, far, projection.T, lcb_grad, *before)


def backward_kernel(grad_ref, first_ref, last_ref, inv_ref, emb_ref, proj_ref, fm_grad_ref):
    n_emb, rank = proj_ref.shape
    width = emb_ref.shape[2]
    per = last_ref.shape[2] // n_emb
    scale = 1.0 / (rank * n_emb)
    at_last = pl.program_id(0) == pl.num_programs(0) - 1

    @pl.when(pl.program_id(0) == 0)
    def _():
        proj_ref[...] = jnp.zeros_like(proj_ref)

    proj = jnp.zeros(proj_ref.shape, jnp.float32)
    for start in range(0, GROUP, ROWS):
        rows = slice(start, start + ROWS)
        grads = [grad_ref[rows, k * n_emb : (k + 1) * n_emb] for k in range(rank)]
        cuts = [(k // per, rows, slice(k % per * n_emb, (k % per + 1) * n_emb)) for k in range(rank)]
        normed = [
            jnp.where(at_last, last_ref[cut].astype(jnp.float32), first_ref[cut].astype(jnp.float32)) for cut in cuts
        ]
        mean = jnp.sum(sum(grads), axis=1, keepdims=True) * scale
        along = jnp.sum(sum(g * x for g, x in zip(grads, normed)), axis=1, keepdims=True) * scale
        inv = inv_ref[rows, :1]
        for k in range(rank):
            fm_grad_ref[pl.ds(k, ROWS, stride=rank), :] = (grads[k] - mean - normed[k] * along) * inv
        for e in range(0, ROWS, 2):
            fm_grad = fm_grad_ref[pl.ds(e * rank, 2 * rank), :].astype(jnp.bfloat16)
            pair = jnp.concatenate([emb_ref[start + e], emb_ref[start + e + 1]], axis=1)
            back = jnp.dot(fm_grad, pair, preferred_element_type=jnp.float32).astype(jnp.bfloat16)
            back = jnp.concatenate([back[:rank, :width], back[rank:, width:]], axis=1)
            proj += lax.dot_general(pair, back, (((1,), (1,)), ((), ())), preferred_element_type=jnp.float32)
    proj_ref[...] += proj


def backward_features(normed_grad, normed_first, normed_last, inv_scale, embedded):
    examples, n_emb, width = embedded.shape
    blocks, count, columns = normed_first.shape
    rank = blocks * columns // n_emb
    firsts = count // GROUP
    assert normed_last.shape[1] == GROUP and count + GROUP == examples
    return pl.pallas_call(
        backward_kernel,
        grid=(firsts + 1,),
        in_specs=[
            pl.BlockSpec((GROUP, rank * n_emb), lambda g: (g, 0)),
            pl.BlockSpec((blocks, GROUP, columns), lambda g: (0, jnp.minimum(g, firsts - 1), 0)),
            pl.BlockSpec((blocks, GROUP, columns), lambda g: (0, 0, 0)),
            pl.BlockSpec((GROUP, 128), lambda g: (g, 0)),
            pl.BlockSpec((GROUP, n_emb, width), lambda g: (g, 0, 0)),
        ],
        out_specs=pl.BlockSpec((n_emb, rank), lambda g: (0, 0)),
        out_shape=jax.ShapeDtypeStruct((n_emb, rank), jnp.float32),
        scratch_shapes=[pltpu.VMEM((ROWS * rank, n_emb), jnp.float32)],
        cost_estimate=pl.CostEstimate(
            flops=40_000_000 * examples,
            bytes_accessed=examples * n_emb * (width * 2 + rank * 6),
            transcendentals=0,
        ),
        name="fm_backward",
    )(normed_grad, normed_first, normed_last, inv_scale, embedded)


def both_cores(half, dims, axes):
    other = swapped(half, "c", 1)
    high = lax.axis_index("c") == 1
    both = [h.reshape(*dims, *half.shape[1:]) for h in (half, other)]
    both = jnp.where(high, jnp.stack(both[::-1]), jnp.stack(both))
    return jnp.transpose(both, axes).reshape(-1, *half.shape[1:])


def per_device(feature_ids, emb_table, factor_machine_projection, mlp_weight, momentum, hidden_grad, lcb_grad):
    mp, zl, y, x, c = (lax.axis_size(a) for a in ("mp", "zl", "y", "x", "c"))
    own = emb_table.shape[0]
    examples, hidden = hidden_grad.shape

    to_worker = []
    for block in range(zl * y * x * c):
        cx, zy = divmod(block, zl * y)
        at_c, at_x = divmod(cx, x)
        to_worker.append((block, (zy * x + at_x) * c + at_c))
    to_owner = [(worker, owner) for owner, worker in to_worker]

    width = emb_table.shape[1]
    table = from_everyone(emb_table, ("mp", "zl")).reshape(-1, width)
    state = lax.ppermute(jnp.stack([mlp_weight, momentum]), DP, to_worker)
    weight_rows, momentum_rows = state[0], state[1]
    weights = mlp_weight.astype(jnp.bfloat16)
    near_rows = table.shape[0]
    table = from_everyone(jnp.concatenate([table, weights[:, :width], weights[:, width:]], axis=0), "y")
    weights = table[:, near_rows:].reshape(y, hidden // width, -1, width)
    weights = jnp.swapaxes(weights, 1, 2).reshape(-1, hidden)
    weights = doubled(weights, "zl", 1)
    weights = jnp.broadcast_to(weights, (x, *weights.shape))
    owner, row = lax.div(feature_ids, own), lax.rem(feature_ids, own)
    owner, at_mp = lax.div(owner, mp), lax.rem(owner, mp)
    owner, at_c = lax.div(owner, c), lax.rem(owner, c)
    owner, at_x = lax.div(owner, x), lax.rem(owner, x)
    at_zl, at_y = lax.div(owner, y), lax.rem(owner, y)
    ids = (((((at_c ^ lax.axis_index("c")) * x + at_x) * y + at_y) * mp + at_mp) * zl + at_zl) * own + row
    table = from_everyone(table[:, :near_rows], "x").reshape(-1, width)
    weights, table = tied(weights, table)
    table_far = swapped(table, "c", 1)
    weights = exchange(weights, "x").reshape(-1, hidden)

    blocks = 2 * c * x
    cut = int(examples * FIRST_SHARE)
    shares = ((0, cut), (cut, examples - cut))
    inputs = (ids, table, table_far, factor_machine_projection, lcb_grad)
    embedded, normed_a, inv_scale, lcb_a = forward_features(*inputs, blocks, *shares[0])
    weights = both_cores(weights, (x, zl, y, mlp_weight.shape[0]), (2, 3, 1, 0, 4, 5))
    embedded, normed_b, inv_scale, lcb_b = forward_features(
        *inputs, blocks, *shares[1], (embedded, inv_scale)
    )
    columns_a = exchange(normed_a.reshape(c * x, 2 * cut, -1), CX)

    tiled_weights = weights.reshape(blocks, -1, hidden)
    preact = jnp.concatenate(
        [
            jnp.einsum("jbk,jkn->bn", normed, tiled_weights, preferred_element_type=jnp.float32)
            for normed in (normed_a, normed_b)
        ],
        axis=0,
    )
    sigmoid_pre = jax.nn.sigmoid(preact)
    preact_grad = (
        hidden_grad.astype(jnp.float32) * sigmoid_pre * (1.0 + preact * (1.0 - sigmoid_pre))
    ).astype(jnp.bfloat16)
    group_grad = exchange(
        jnp.concatenate(
            [
                jnp.broadcast_to(preact_grad, (c * x, examples, hidden)),
                normed_b.reshape(c * x, -1, hidden),
            ],
            axis=1,
        ),
        CX,
    )

    normed_part = lax.dot_general(preact_grad, weights, (((1,), (1,)), ((), ())), preferred_element_type=jnp.float32)
    proj_part = backward_features(normed_part, normed_a, normed_b, inv_scale, embedded)
    (start_a, count_a), (start_b, count_b) = shares
    weight_grad = jnp.einsum(
        "shbk,sbn->hkn",
        columns_a.reshape(c * x, 2, count_a, -1),
        group_grad[:, :count_a],
        preferred_element_type=jnp.float32,
    ) + jnp.stack(
        [
            jnp.einsum(
                "sbk,sbn->kn",
                group_grad[:, at : at + count_b],
                group_grad[:, start_b:examples],
                preferred_element_type=jnp.float32,
            )
            for at in (examples, examples + count_b)
        ]
    )
    arrived = exchange(weight_grad.astype(jnp.bfloat16).reshape(zl * y, -1, hidden), ZY)
    small = proj_part.T
    small += swapped(small, "mp", 1)
    small += swapped(small, "mp", 3)
    small = jnp.concatenate([small, lcb_a + lcb_b], axis=1)
    arrived, small = tied(arrived, small)
    new_momentum = 0.9 * momentum_rows + summed(arrived)
    new_weight = weight_rows - 0.01 * new_momentum
    own_rows = new_weight.shape[0]
    arrived = from_everyone(jnp.concatenate([new_weight, small], axis=0).astype(jnp.bfloat16), ZY)
    next_weight = arrived[:, :own_rows].reshape(-1, hidden)
    small = in_two_parts(summed(arrived[:, own_rows:]))
    column_rows = next_weight.shape[0]
    arrived = from_everyone(jnp.concatenate([next_weight, small], axis=0), "x")
    state = lax.ppermute(jnp.stack([new_weight, new_momentum]), DP, to_owner)
    arrived, state = tied(arrived, state)
    other = swapped(arrived, "c", 1)
    high = lax.axis_index("c") == 1
    halves = [h[:, :column_rows] for h in (arrived, other)]
    next_weight = jnp.where(high, jnp.stack(halves[::-1]), jnp.stack(halves)).reshape(-1, hidden)
    small = [summed(h[:, column_rows:].reshape(2 * x, -1, hidden)) for h in (arrived, other)]
    small = small[0] + small[1]
    n_emb = small.shape[1] // 2
    return (state[0], state[1], next_weight, small[:, :n_emb].T, small[:, n_emb:].T)


def solution(mesh):
    torus = Mesh(mesh.devices.reshape(2, 8, 4, 2, mesh.shape["mp"]), DP_MP)
    placed = (
        P(DP, None),
        P(DP_MP, None),
        P(),
        P(DP, "mp"),
        P(DP, "mp"),
        P(DP, "mp"),
        P(DP, "mp", None),
    )

    return jax.shard_map(
        per_device,
        mesh=torus,
        in_specs=placed,
        out_specs=(P(DP, "mp"), P(DP, "mp"), P(None, "mp"), P(), P(None, "mp")),
        check_vma=False,
    )
```

```python
import jax
import jax.numpy as jnp
from jax import lax
from jax.experimental import pallas as pl
from jax.experimental.pallas import tpu as pltpu
from jax.sharding import Mesh
from jax.sharding import PartitionSpec as P


DP = ("zl", "y", "x", "c")
DP_MP = ("zl", "y", "x", "c", "mp")
CX = ("c", "x")
ZY = ("zl", "y")
GROUP = 32
ROWS = 8
FIRST_SHARE = 0.75


def exchange(tiles, axis):
    return lax.all_to_all(tiles, axis, split_axis=0, concat_axis=0, tiled=True)


def from_everyone(x, axis):
    return exchange(jnp.broadcast_to(x, (lax.axis_size(axis), *x.shape)), axis)


def swapped(x, axis, flip):
    return lax.ppermute(x, axis, [(i, i ^ flip) for i in range(lax.axis_size(axis))])


def in_two_parts(x):
    first = lax.reduce_precision(x, 8, 7)
    return jnp.concatenate([first, x - first], axis=0).astype(jnp.bfloat16)


def doubled(x, axis, flip):
    other = swapped(x, axis, flip)
    high = (lax.axis_index(axis) & flip) != 0
    return jnp.concatenate([jnp.where(high, other, x), jnp.where(high, x, other)], axis=0)


def tied(*values):
    return lax.optimization_barrier(values)


def summed(tiles):
    return tiles.astype(jnp.float32).sum(axis=0)


def forward_kernel(ids_ref, near_ref, far_ref, proj_ref, lcb_ref, *refs):
    emb_ref, normed_ref, inv_ref, lcb_sum_ref, table_ref, even_ref, odd_ref, fm_ref = refs[-8:]
    rank, n_emb = proj_ref.shape
    half, width = near_ref.shape

    @pl.when(pl.program_id(0) == 0)
    def _():
        lcb_sum_ref[...] = jnp.zeros_like(lcb_sum_ref)

        @pl.loop(0, half // 128)
        def _(i):
            at = pl.multiple_of(i * 128, 128)
            table_ref[pl.ds(at, 128), :] = near_ref[pl.ds(at, 128), :].astype(jnp.float32)
            table_ref[pl.ds(half + at, 128), :] = far_ref[pl.ds(at, 128), :].astype(jnp.float32)

    proj = proj_ref[...]
    scale = 1.0 / (rank * n_emb)
    per = normed_ref.shape[2] // n_emb
    outputs = lcb_ref.shape[1]
    lcb_sum = jnp.zeros(lcb_sum_ref.shape, jnp.float32)
    for start in range(0, GROUP, ROWS):
        for e in range(0, ROWS, 2):
            rows_ref = (even_ref, odd_ref)[e // 2 % 2]
            for r in range(2 * n_emb):
                row = ids_ref[start + e + r // n_emb, r % n_emb]
                rows_ref[pl.ds(r, 1), :] = table_ref[pl.ds(row, 1), :]
            pair = rows_ref[...].astype(jnp.bfloat16)
            first, second = pair[:n_emb], pair[n_emb:]
            emb_ref[start + e] = first
            emb_ref[start + e + 1] = second
            compressed = jnp.dot(
                proj, jnp.concatenate([first, second], axis=1), preferred_element_type=jnp.float32
            ).astype(jnp.bfloat16)
            left = jnp.concatenate(
                [compressed[:, :width], compressed[:, width:], lcb_ref[start + e], lcb_ref[start + e + 1]], axis=0
            )
            fm = lax.dot_general(left, pair, (((1,), (1,)), ((), ())), preferred_element_type=jnp.float32)
            fm_ref[pl.ds(e * rank, rank), :] = fm[:rank, :n_emb]
            fm_ref[pl.ds((e + 1) * rank, rank), :] = fm[rank : 2 * rank, n_emb:]
            lcb_sum += fm[2 * rank : 2 * rank + outputs, :n_emb] + fm[2 * rank + outputs :, n_emb:]
        parts = [fm_ref[pl.ds(k, ROWS, stride=rank), :] for k in range(rank)]
        mean = jnp.sum(sum(parts), axis=1, keepdims=True) * scale
        parts = [p - mean for p in parts]
        var = jnp.sum(sum(p * p for p in parts), axis=1, keepdims=True) * scale
        inv = 1.0 / jnp.sqrt(var + 1.0)
        for k in range(rank):
            at = k % per * n_emb
            normed_ref[k // per, start : start + ROWS, at : at + n_emb] = (parts[k] * inv).astype(jnp.bfloat16)
        inv_ref[start : start + ROWS] = jnp.broadcast_to(inv, (ROWS, inv_ref.shape[1]))
    lcb_sum_ref[...] += lcb_sum


def forward_features(ids, near, far, projection, lcb_grad, blocks, start, count, before=()):
    examples, n_emb = ids.shape
    half, width = near.shape
    rank = projection.shape[1]
    columns = rank * n_emb // blocks
    skip = start // GROUP
    outputs = lcb_grad.shape[1]
    return pl.pallas_call(
        forward_kernel,
        grid=(count // GROUP,),
        in_specs=[
            pl.BlockSpec((GROUP, n_emb), lambda g: (g + skip, 0), memory_space=pltpu.SMEM),
            pl.BlockSpec((half, width), lambda g: (0, 0)),
            pl.BlockSpec((half, width), lambda g: (0, 0)),
            pl.BlockSpec((rank, n_emb), lambda g: (0, 0)),
            pl.BlockSpec((GROUP, outputs, width), lambda g: (g + skip, 0, 0)),
            *(pl.BlockSpec(memory_space=pl.ANY) for _ in before),
        ],
        out_specs=[
            pl.BlockSpec((GROUP, n_emb, width), lambda g: (g + skip, 0, 0)),
            pl.BlockSpec((blocks, GROUP, columns), lambda g: (0, g, 0)),
            pl.BlockSpec((GROUP, 128), lambda g: (g + skip, 0)),
            pl.BlockSpec((outputs, n_emb), lambda g: (0, 0)),
        ],
        out_shape=[
            jax.ShapeDtypeStruct((examples, n_emb, width), jnp.bfloat16),
            jax.ShapeDtypeStruct((blocks, count, columns), jnp.bfloat16),
            jax.ShapeDtypeStruct((examples, 128), jnp.float32),
            jax.ShapeDtypeStruct((outputs, n_emb), jnp.float32),
        ],
        scratch_shapes=[
            pltpu.VMEM((2 * half, width), jnp.float32),
            pltpu.VMEM((2 * n_emb, width), jnp.float32),
            pltpu.VMEM((2 * n_emb, width), jnp.float32),
            pltpu.VMEM((ROWS * rank, n_emb), jnp.float32),
        ],
        input_output_aliases={5: 0, 6: 2} if before else {},
        cost_estimate=pl.CostEstimate(
            flops=100_000_000 * count,
            bytes_accessed=half * width * 4 + count * n_emb * width * 2,
            transcendentals=0,
        ),
        name="fm_forward",
    )(ids, near, far, projection.T, lcb_grad, *before)


def backward_kernel(grad_ref, first_ref, last_ref, inv_ref, emb_ref, proj_ref, fm_grad_ref):
    n_emb, rank = proj_ref.shape
    width = emb_ref.shape[2]
    per = last_ref.shape[2] // n_emb
    scale = 1.0 / (rank * n_emb)
    at_last = pl.program_id(0) == pl.num_programs(0) - 1

    @pl.when(pl.program_id(0) == 0)
    def _():
        proj_ref[...] = jnp.zeros_like(proj_ref)

    proj = jnp.zeros(proj_ref.shape, jnp.float32)
    for start in range(0, GROUP, ROWS):
        rows = slice(start, start + ROWS)
        grads = [grad_ref[rows, k * n_emb : (k + 1) * n_emb] for k in range(rank)]
        cuts = [(k // per, rows, slice(k % per * n_emb, (k % per + 1) * n_emb)) for k in range(rank)]
        normed = [
            jnp.where(at_last, last_ref[cut].astype(jnp.float32), first_ref[cut].astype(jnp.float32)) for cut in cuts
        ]
        mean = jnp.sum(sum(grads), axis=1, keepdims=True) * scale
        along = jnp.sum(sum(g * x for g, x in zip(grads, normed)), axis=1, keepdims=True) * scale
        inv = inv_ref[rows, :1]
        for k in range(rank):
            fm_grad_ref[pl.ds(k, ROWS, stride=rank), :] = (grads[k] - mean - normed[k] * along) * inv
        pairs, backs = [], []
        for e in range(0, ROWS, 2):
            fm_grad = fm_grad_ref[pl.ds(e * rank, 2 * rank), :].astype(jnp.bfloat16)
            pair = jnp.concatenate([emb_ref[start + e], emb_ref[start + e + 1]], axis=1)
            back = jnp.dot(fm_grad, pair, preferred_element_type=jnp.float32).astype(jnp.bfloat16)
            pairs.append(pair)
            backs += [back[:rank, :width], back[rank:, width:]]
        proj += lax.dot_general(
            jnp.concatenate(pairs, axis=1),
            jnp.concatenate(backs, axis=1),
            (((1,), (1,)), ((), ())),
            preferred_element_type=jnp.float32,
        )
    proj_ref[...] += proj


def backward_features(normed_grad, normed_first, normed_last, inv_scale, embedded):
    examples, n_emb, width = embedded.shape
    blocks, count, columns = normed_first.shape
    rank = blocks * columns // n_emb
    firsts = count // GROUP
    assert normed_last.shape[1] == GROUP and count + GROUP == examples
    return pl.pallas_call(
        backward_kernel,
        grid=(firsts + 1,),
        in_specs=[
            pl.BlockSpec((GROUP, rank * n_emb), lambda g: (g, 0)),
            pl.BlockSpec((blocks, GROUP, columns), lambda g: (0, jnp.minimum(g, firsts - 1), 0)),
            pl.BlockSpec((blocks, GROUP, columns), lambda g: (0, 0, 0)),
            pl.BlockSpec((GROUP, 128), lambda g: (g, 0)),
            pl.BlockSpec((GROUP, n_emb, width), lambda g: (g, 0, 0)),
        ],
        out_specs=pl.BlockSpec((n_emb, rank), lambda g: (0, 0)),
        out_shape=jax.ShapeDtypeStruct((n_emb, rank), jnp.float32),
        scratch_shapes=[pltpu.VMEM((ROWS * rank, n_emb), jnp.float32)],
        cost_estimate=pl.CostEstimate(
            flops=40_000_000 * examples,
            bytes_accessed=examples * n_emb * (width * 2 + rank * 6),
            transcendentals=0,
        ),
        name="fm_backward",
    )(normed_grad, normed_first, normed_last, inv_scale, embedded)


def both_cores(half, dims, axes):
    other = swapped(half, "c", 1)
    high = lax.axis_index("c") == 1
    both = [h.reshape(*dims, *half.shape[1:]) for h in (half, other)]
    both = jnp.where(high, jnp.stack(both[::-1]), jnp.stack(both))
    return jnp.transpose(both, axes).reshape(-1, *half.shape[1:])


def per_device(feature_ids, emb_table, factor_machine_projection, mlp_weight, momentum, hidden_grad, lcb_grad):
    mp, zl, y, x, c = (lax.axis_size(a) for a in ("mp", "zl", "y", "x", "c"))
    own = emb_table.shape[0]
    examples, hidden = hidden_grad.shape

    to_worker = []
    for block in range(zl * y * x * c):
        cx, zy = divmod(block, zl * y)
        at_c, at_x = divmod(cx, x)
        to_worker.append((block, (zy * x + at_x) * c + at_c))
    to_owner = [(worker, owner) for owner, worker in to_worker]

    width = emb_table.shape[1]
    table = from_everyone(emb_table, ("mp", "zl")).reshape(-1, width)
    state = lax.ppermute(jnp.stack([mlp_weight, momentum]), DP, to_worker)
    weight_rows, momentum_rows = state[0], state[1]
    weights = mlp_weight.astype(jnp.bfloat16)
    near_rows = table.shape[0]
    table = from_everyone(jnp.concatenate([table, weights[:, :width], weights[:, width:]], axis=0), "y")
    weights = table[:, near_rows:].reshape(y, hidden // width, -1, width)
    weights = jnp.swapaxes(weights, 1, 2).reshape(-1, hidden)
    weights = doubled(weights, "zl", 1)
    weights = jnp.broadcast_to(weights, (x, *weights.shape))
    owner, row = lax.div(feature_ids, own), lax.rem(feature_ids, own)
    owner, at_mp = lax.div(owner, mp), lax.rem(owner, mp)
    owner, at_c = lax.div(owner, c), lax.rem(owner, c)
    owner, at_x = lax.div(owner, x), lax.rem(owner, x)
    at_zl, at_y = lax.div(owner, y), lax.rem(owner, y)
    ids = (((((at_c ^ lax.axis_index("c")) * x + at_x) * y + at_y) * mp + at_mp) * zl + at_zl) * own + row
    table = from_everyone(table[:, :near_rows], "x").reshape(-1, width)
    weights, table = tied(weights, table)
    table_far = swapped(table, "c", 1)
    weights = exchange(weights, "x").reshape(-1, hidden)

    blocks = 2 * c * x
    cut = int(examples * FIRST_SHARE)
    shares = ((0, cut), (cut, examples - cut))
    inputs = (ids, table, table_far, factor_machine_projection, lcb_grad)
    embedded, normed_a, inv_scale, lcb_a = forward_features(*inputs, blocks, *shares[0])
    weights = both_cores(weights, (x, zl, y, mlp_weight.shape[0]), (2, 3, 1, 0, 4, 5))
    embedded, normed_b, inv_scale, lcb_b = forward_features(
        *inputs, blocks, *shares[1], (embedded, inv_scale)
    )
    columns_a = exchange(normed_a.reshape(c * x, 2 * cut, -1), CX)

    tiled_weights = weights.reshape(blocks, -1, hidden)
    preact = jnp.concatenate(
        [
            jnp.einsum("jbk,jkn->bn", normed, tiled_weights, preferred_element_type=jnp.float32)
            for normed in (normed_a, normed_b)
        ],
        axis=0,
    )
    sigmoid_pre = jax.nn.sigmoid(preact)
    preact_grad = (
        hidden_grad.astype(jnp.float32) * sigmoid_pre * (1.0 + preact * (1.0 - sigmoid_pre))
    ).astype(jnp.bfloat16)
    group_grad = exchange(
        jnp.concatenate(
            [
                jnp.broadcast_to(preact_grad, (c * x, examples, hidden)),
                normed_b.reshape(c * x, -1, hidden),
            ],
            axis=1,
        ),
        CX,
    )

    normed_part = lax.dot_general(preact_grad, weights, (((1,), (1,)), ((), ())), preferred_element_type=jnp.float32)
    proj_part = backward_features(normed_part, normed_a, normed_b, inv_scale, embedded)
    (start_a, count_a), (start_b, count_b) = shares
    weight_grad = jnp.einsum(
        "shbk,sbn->hkn",
        columns_a.reshape(c * x, 2, count_a, -1),
        group_grad[:, :count_a],
        preferred_element_type=jnp.float32,
    ) + jnp.stack(
        [
            jnp.einsum(
                "sbk,sbn->kn",
                group_grad[:, at : at + count_b],
                group_grad[:, start_b:examples],
                preferred_element_type=jnp.float32,
            )
            for at in (examples, examples + count_b)
        ]
    )
    arrived = exchange(weight_grad.astype(jnp.bfloat16).reshape(zl * y, -1, hidden), ZY)
    small = proj_part.T
    small += swapped(small, "mp", 1)
    small += swapped(small, "mp", 3)
    small = jnp.concatenate([small, lcb_a + lcb_b], axis=1)
    arrived, small = tied(arrived, small)
    new_momentum = 0.9 * momentum_rows + summed(arrived)
    new_weight = weight_rows - 0.01 * new_momentum
    own_rows = new_weight.shape[0]
    arrived = from_everyone(jnp.concatenate([new_weight, small], axis=0).astype(jnp.bfloat16), ZY)
    next_weight = arrived[:, :own_rows].reshape(-1, hidden)
    small = in_two_parts(summed(arrived[:, own_rows:]))
    column_rows = next_weight.shape[0]
    arrived = from_everyone(jnp.concatenate([next_weight, small], axis=0), "x")
    state = lax.ppermute(jnp.stack([new_weight, new_momentum]), DP, to_owner)
    arrived, state = tied(arrived, state)
    other = swapped(arrived, "c", 1)
    high = lax.axis_index("c") == 1
    halves = [h[:, :column_rows] for h in (arrived, other)]
    next_weight = jnp.where(high, jnp.stack(halves[::-1]), jnp.stack(halves)).reshape(-1, hidden)
    small = [summed(h[:, column_rows:].reshape(2 * x, -1, hidden)) for h in (arrived, other)]
    small = small[0] + small[1]
    n_emb = small.shape[1] // 2
    return (state[0], state[1], next_weight, small[:, :n_emb].T, small[:, n_emb:].T)


def solution(mesh):
    torus = Mesh(mesh.devices.reshape(2, 8, 4, 2, mesh.shape["mp"]), DP_MP)
    placed = (
        P(DP, None),
        P(DP_MP, None),
        P(),
        P(DP, "mp"),
        P(DP, "mp"),
        P(DP, "mp"),
        P(DP, "mp", None),
    )

    return jax.shard_map(
        per_device,
        mesh=torus,
        in_specs=placed,
        out_specs=(P(DP, "mp"), P(DP, "mp"), P(None, "mp"), P(), P(None, "mp")),
        check_vma=False,
    )
```

```python
import jax
import jax.numpy as jnp
from jax import lax
from jax.experimental import pallas as pl
from jax.experimental.pallas import tpu as pltpu
from jax.sharding import Mesh
from jax.sharding import PartitionSpec as P


DP = ("zl", "y", "x", "c")
DP_MP = ("zl", "y", "x", "c", "mp")
CX = ("c", "x")
ZY = ("zl", "y")
GROUP = 32
ROWS = 8
FIRST_SHARE = 0.75


def exchange(tiles, axis):
    return lax.all_to_all(tiles, axis, split_axis=0, concat_axis=0, tiled=True)


def from_everyone(x, axis):
    return exchange(jnp.broadcast_to(x, (lax.axis_size(axis), *x.shape)), axis)


def swapped(x, axis, flip):
    return lax.ppermute(x, axis, [(i, i ^ flip) for i in range(lax.axis_size(axis))])


def in_two_parts(x):
    first = lax.reduce_precision(x, 8, 7)
    return jnp.concatenate([first, x - first], axis=0).astype(jnp.bfloat16)


def doubled(x, axis, flip):
    other = swapped(x, axis, flip)
    high = (lax.axis_index(axis) & flip) != 0
    return jnp.concatenate([jnp.where(high, other, x), jnp.where(high, x, other)], axis=0)


def tied(*values):
    return lax.optimization_barrier(values)


def summed(tiles):
    return tiles.astype(jnp.float32).sum(axis=0)


def forward_kernel(ids_ref, near_ref, far_ref, proj_ref, lcb_ref, *refs):
    emb_ref, normed_ref, inv_ref, lcb_sum_ref, table_ref, even_ref, odd_ref, fm_ref = refs[-8:]
    rank, n_emb = proj_ref.shape
    half, width = near_ref.shape

    @pl.when(pl.program_id(0) == 0)
    def _():
        lcb_sum_ref[...] = jnp.zeros_like(lcb_sum_ref)

        @pl.loop(0, half // 128)
        def _(i):
            at = pl.multiple_of(i * 128, 128)
            table_ref[pl.ds(at, 128), :] = near_ref[pl.ds(at, 128), :].astype(jnp.float32)
            table_ref[pl.ds(half + at, 128), :] = far_ref[pl.ds(at, 128), :].astype(jnp.float32)

    proj = proj_ref[...]
    scale = 1.0 / (rank * n_emb)
    per = normed_ref.shape[2] // n_emb
    outputs = lcb_ref.shape[1]
    lcb_sum = jnp.zeros(lcb_sum_ref.shape, jnp.float32)
    for start in range(0, GROUP, ROWS):
        for e in range(0, ROWS, 2):
            rows_ref = (even_ref, odd_ref)[e // 2 % 2]
            for r in range(2 * n_emb):
                row = ids_ref[start + e + r // n_emb, r % n_emb]
                rows_ref[pl.ds(r, 1), :] = table_ref[pl.ds(row, 1), :]
            pair = rows_ref[...].astype(jnp.bfloat16)
            first, second = pair[:n_emb], pair[n_emb:]
            emb_ref[start + e] = first
            emb_ref[start + e + 1] = second
            compressed = jnp.dot(
                proj, jnp.concatenate([first, second], axis=1), preferred_element_type=jnp.float32
            ).astype(jnp.bfloat16)
            left = jnp.concatenate(
                [compressed[:, :width], compressed[:, width:], lcb_ref[start + e], lcb_ref[start + e + 1]], axis=0
            )
            fm = lax.dot_general(left, pair, (((1,), (1,)), ((), ())), preferred_element_type=jnp.float32)
            fm_ref[pl.ds(e * rank, rank), :] = fm[:rank, :n_emb]
            fm_ref[pl.ds((e + 1) * rank, rank), :] = fm[rank : 2 * rank, n_emb:]
            lcb_sum += fm[2 * rank : 2 * rank + outputs, :n_emb] + fm[2 * rank + outputs :, n_emb:]
        parts = [fm_ref[pl.ds(k, ROWS, stride=rank), :] for k in range(rank)]
        mean = jnp.sum(sum(parts), axis=1, keepdims=True) * scale
        parts = [p - mean for p in parts]
        var = jnp.sum(sum(p * p for p in parts), axis=1, keepdims=True) * scale
        inv = 1.0 / jnp.sqrt(var + 1.0)
        for k in range(rank):
            at = k % per * n_emb
            normed_ref[k // per, start : start + ROWS, at : at + n_emb] = (parts[k] * inv).astype(jnp.bfloat16)
        inv_ref[start : start + ROWS] = jnp.broadcast_to(inv, (ROWS, inv_ref.shape[1]))
    lcb_sum_ref[...] += lcb_sum


def forward_features(ids, near, far, projection, lcb_grad, blocks, start, count, before=()):
    examples, n_emb = ids.shape
    half, width = near.shape
    rank = projection.shape[1]
    columns = rank * n_emb // blocks
    skip = start // GROUP
    outputs = lcb_grad.shape[1]
    return pl.pallas_call(
        forward_kernel,
        grid=(count // GROUP,),
        in_specs=[
            pl.BlockSpec((GROUP, n_emb), lambda g: (g + skip, 0), memory_space=pltpu.SMEM),
            pl.BlockSpec((half, width), lambda g: (0, 0)),
            pl.BlockSpec((half, width), lambda g: (0, 0)),
            pl.BlockSpec((rank, n_emb), lambda g: (0, 0)),
            pl.BlockSpec((GROUP, outputs, width), lambda g: (g + skip, 0, 0)),
            *(pl.BlockSpec(memory_space=pl.ANY) for _ in before),
        ],
        out_specs=[
            pl.BlockSpec((GROUP, n_emb, width), lambda g: (g + skip, 0, 0)),
            pl.BlockSpec((blocks, GROUP, columns), lambda g: (0, g, 0)),
            pl.BlockSpec((GROUP, 128), lambda g: (g + skip, 0)),
            pl.BlockSpec((outputs, n_emb), lambda g: (0, 0)),
        ],
        out_shape=[
            jax.ShapeDtypeStruct((examples, n_emb, width), jnp.bfloat16),
            jax.ShapeDtypeStruct((blocks, count, columns), jnp.bfloat16),
            jax.ShapeDtypeStruct((examples, 128), jnp.float32),
            jax.ShapeDtypeStruct((outputs, n_emb), jnp.float32),
        ],
        scratch_shapes=[
            pltpu.VMEM((2 * half, width), jnp.float32),
            pltpu.VMEM((2 * n_emb, width), jnp.float32),
            pltpu.VMEM((2 * n_emb, width), jnp.float32),
            pltpu.VMEM((ROWS * rank, n_emb), jnp.float32),
        ],
        input_output_aliases={5: 0, 6: 2} if before else {},
        cost_estimate=pl.CostEstimate(
            flops=100_000_000 * count,
            bytes_accessed=half * width * 4 + count * n_emb * width * 2,
            transcendentals=0,
        ),
        name="fm_forward",
    )(ids, near, far, projection.T, lcb_grad, *before)


def backward_kernel(grad_ref, first_ref, last_ref, inv_ref, emb_ref, proj_ref, fm_grad_ref):
    n_emb, rank = proj_ref.shape
    width = emb_ref.shape[2]
    per = last_ref.shape[2] // n_emb
    scale = 1.0 / (rank * n_emb)
    at_last = pl.program_id(0) == pl.num_programs(0) - 1

    @pl.when(pl.program_id(0) == 0)
    def _():
        proj_ref[...] = jnp.zeros_like(proj_ref)

    proj = jnp.zeros(proj_ref.shape, jnp.float32)
    for start in range(0, GROUP, ROWS):
        rows = slice(start, start + ROWS)
        grads = [grad_ref[rows, k * n_emb : (k + 1) * n_emb] for k in range(rank)]
        cuts = [(k // per, rows, slice(k % per * n_emb, (k % per + 1) * n_emb)) for k in range(rank)]
        normed = [
            jnp.where(at_last, last_ref[cut].astype(jnp.float32), first_ref[cut].astype(jnp.float32)) for cut in cuts
        ]
        mean = jnp.sum(sum(grads), axis=1, keepdims=True) * scale
        along = jnp.sum(sum(g * x for g, x in zip(grads, normed)), axis=1, keepdims=True) * scale
        inv = inv_ref[rows, :1]
        for k in range(rank):
            fm_grad_ref[pl.ds(k, ROWS, stride=rank), :] = (grads[k] - mean - normed[k] * along) * inv
        pairs, backs = [], []
        for e in range(0, ROWS, 2):
            fm_grad = fm_grad_ref[pl.ds(e * rank, 2 * rank), :].astype(jnp.bfloat16)
            pair = jnp.concatenate([emb_ref[start + e], emb_ref[start + e + 1]], axis=1)
            back = jnp.dot(fm_grad, pair, preferred_element_type=jnp.float32).astype(jnp.bfloat16)
            pairs.append(pair)
            backs += [back[:rank, :width], back[rank:, width:]]
        proj += lax.dot_general(
            jnp.concatenate(pairs, axis=1),
            jnp.concatenate(backs, axis=1),
            (((1,), (1,)), ((), ())),
            preferred_element_type=jnp.float32,
        )
    proj_ref[...] += proj


def backward_features(normed_grad, normed_first, normed_last, inv_scale, embedded):
    examples, n_emb, width = embedded.shape
    blocks, count, columns = normed_first.shape
    rank = blocks * columns // n_emb
    firsts = count // GROUP
    assert normed_last.shape[1] == GROUP and count + GROUP == examples
    return pl.pallas_call(
        backward_kernel,
        grid=(firsts + 1,),
        in_specs=[
            pl.BlockSpec((GROUP, rank * n_emb), lambda g: (g, 0)),
            pl.BlockSpec((blocks, GROUP, columns), lambda g: (0, jnp.minimum(g, firsts - 1), 0)),
            pl.BlockSpec((blocks, GROUP, columns), lambda g: (0, 0, 0)),
            pl.BlockSpec((GROUP, 128), lambda g: (g, 0)),
            pl.BlockSpec((GROUP, n_emb, width), lambda g: (g, 0, 0)),
        ],
        out_specs=pl.BlockSpec((n_emb, rank), lambda g: (0, 0)),
        out_shape=jax.ShapeDtypeStruct((n_emb, rank), jnp.float32),
        scratch_shapes=[pltpu.VMEM((ROWS * rank, n_emb), jnp.float32)],
        cost_estimate=pl.CostEstimate(
            flops=40_000_000 * examples,
            bytes_accessed=examples * n_emb * (width * 2 + rank * 6),
            transcendentals=0,
        ),
        name="fm_backward",
    )(normed_grad, normed_first, normed_last, inv_scale, embedded)


def both_cores(half, dims, axes):
    other = swapped(half, "c", 1)
    high = lax.axis_index("c") == 1
    both = [h.reshape(*dims, *half.shape[1:]) for h in (half, other)]
    both = jnp.where(high, jnp.stack(both[::-1]), jnp.stack(both))
    return jnp.transpose(both, axes).reshape(-1, *half.shape[1:])


def per_device(feature_ids, emb_table, factor_machine_projection, mlp_weight, momentum, hidden_grad, lcb_grad):
    mp, zl, y, x, c = (lax.axis_size(a) for a in ("mp", "zl", "y", "x", "c"))
    own = emb_table.shape[0]
    examples, hidden = hidden_grad.shape

    to_worker = []
    for block in range(zl * y * x * c):
        cx, zy = divmod(block, zl * y)
        at_c, at_x = divmod(cx, x)
        to_worker.append((block, (zy * x + at_x) * c + at_c))
    to_owner = [(worker, owner) for owner, worker in to_worker]

    width = emb_table.shape[1]
    weights = mlp_weight.astype(jnp.bfloat16)
    table = from_everyone(jnp.concatenate([emb_table, weights[:, :width], weights[:, width:]], axis=0), "y")
    weights = table[:, own:].reshape(y, hidden // width, -1, width)
    weights = jnp.swapaxes(weights, 1, 2).reshape(-1, hidden)
    table = from_everyone(table[:, :own].reshape(-1, width), ("mp", "zl")).reshape(-1, width)
    state = lax.ppermute(jnp.stack([mlp_weight, momentum]), DP, to_worker)
    weight_rows, momentum_rows = state[0], state[1]
    weights = doubled(weights, "zl", 1)
    weights = jnp.broadcast_to(weights, (x, *weights.shape))
    owner, row = lax.div(feature_ids, own), lax.rem(feature_ids, own)
    owner, at_mp = lax.div(owner, mp), lax.rem(owner, mp)
    owner, at_c = lax.div(owner, c), lax.rem(owner, c)
    owner, at_x = lax.div(owner, x), lax.rem(owner, x)
    at_zl, at_y = lax.div(owner, y), lax.rem(owner, y)
    ids = (((((at_c ^ lax.axis_index("c")) * x + at_x) * mp + at_mp) * zl + at_zl) * y + at_y) * own + row
    table = from_everyone(table, "x").reshape(-1, width)
    weights, table = tied(weights, table)
    table_far = swapped(table, "c", 1)
    weights = exchange(weights, "x").reshape(-1, hidden)

    blocks = 2 * c * x
    cut = int(examples * FIRST_SHARE)
    shares = ((0, cut), (cut, examples - cut))
    inputs = (ids, table, table_far, factor_machine_projection, lcb_grad)
    embedded, normed_a, inv_scale, lcb_a = forward_features(*inputs, blocks, *shares[0])
    weights = both_cores(weights, (x, zl, y, mlp_weight.shape[0]), (2, 3, 1, 0, 4, 5))
    embedded, normed_b, inv_scale, lcb_b = forward_features(
        *inputs, blocks, *shares[1], (embedded, inv_scale)
    )
    columns_a = exchange(normed_a.reshape(c * x, 2 * cut, -1), CX)

    tiled_weights = weights.reshape(blocks, -1, hidden)
    preact = jnp.concatenate(
        [
            jnp.einsum("jbk,jkn->bn", normed, tiled_weights, preferred_element_type=jnp.float32)
            for normed in (normed_a, normed_b)
        ],
        axis=0,
    )
    sigmoid_pre = jax.nn.sigmoid(preact)
    preact_grad = (
        hidden_grad.astype(jnp.float32) * sigmoid_pre * (1.0 + preact * (1.0 - sigmoid_pre))
    ).astype(jnp.bfloat16)
    group_grad = exchange(
        jnp.concatenate(
            [
                jnp.broadcast_to(preact_grad, (c * x, examples, hidden)),
                normed_b.reshape(c * x, -1, hidden),
            ],
            axis=1,
        ),
        CX,
    )

    normed_part = lax.dot_general(preact_grad, weights, (((1,), (1,)), ((), ())), preferred_element_type=jnp.float32)
    proj_part = backward_features(normed_part, normed_a, normed_b, inv_scale, embedded)
    (start_a, count_a), (start_b, count_b) = shares
    weight_grad = jnp.einsum(
        "shbk,sbn->hkn",
        columns_a.reshape(c * x, 2, count_a, -1),
        group_grad[:, :count_a],
        preferred_element_type=jnp.float32,
    ) + jnp.stack(
        [
            jnp.einsum(
                "sbk,sbn->kn",
                group_grad[:, at : at + count_b],
                group_grad[:, start_b:examples],
                preferred_element_type=jnp.float32,
            )
            for at in (examples, examples + count_b)
        ]
    )
    arrived = exchange(weight_grad.astype(jnp.bfloat16).reshape(zl * y, -1, hidden), ZY)
    small = proj_part.T
    small += swapped(small, "mp", 1)
    small += swapped(small, "mp", 3)
    small = jnp.concatenate([small, lcb_a + lcb_b], axis=1)
    arrived, small = tied(arrived, small)
    new_momentum = 0.9 * momentum_rows + summed(arrived)
    new_weight = weight_rows - 0.01 * new_momentum
    own_rows = new_weight.shape[0]
    arrived = from_everyone(jnp.concatenate([new_weight, small], axis=0).astype(jnp.bfloat16), ZY)
    next_weight = arrived[:, :own_rows].reshape(-1, hidden)
    small = in_two_parts(summed(arrived[:, own_rows:]))
    column_rows = next_weight.shape[0]
    arrived = from_everyone(jnp.concatenate([next_weight, small], axis=0), "x")
    state = lax.ppermute(jnp.stack([new_weight, new_momentum]), DP, to_owner)
    arrived, state = tied(arrived, state)
    other = swapped(arrived, "c", 1)
    high = lax.axis_index("c") == 1
    halves = [h[:, :column_rows] for h in (arrived, other)]
    next_weight = jnp.where(high, jnp.stack(halves[::-1]), jnp.stack(halves)).reshape(-1, hidden)
    small = [summed(h[:, column_rows:].reshape(2 * x, -1, hidden)) for h in (arrived, other)]
    small = small[0] + small[1]
    n_emb = small.shape[1] // 2
    return (state[0], state[1], next_weight, small[:, :n_emb].T, small[:, n_emb:].T)


def solution(mesh):
    torus = Mesh(mesh.devices.reshape(2, 8, 4, 2, mesh.shape["mp"]), DP_MP)
    placed = (
        P(DP, None),
        P(DP_MP, None),
        P(),
        P(DP, "mp"),
        P(DP, "mp"),
        P(DP, "mp"),
        P(DP, "mp", None),
    )

    return jax.shard_map(
        per_device,
        mesh=torus,
        in_specs=placed,
        out_specs=(P(DP, "mp"), P(DP, "mp"), P(None, "mp"), P(), P(None, "mp")),
        check_vma=False,
    )
```

```python
import jax
import jax.numpy as jnp
from jax import lax
from jax.experimental import pallas as pl
from jax.experimental.pallas import tpu as pltpu
from jax.sharding import Mesh
from jax.sharding import PartitionSpec as P


DP = ("zl", "y", "x", "c")
DP_MP = ("zl", "y", "x", "c", "mp")
CX = ("c", "x")
ZY = ("zl", "y")
GROUP = 32
ROWS = 8
FIRST_SHARE = 0.75


def exchange(tiles, axis):
    return lax.all_to_all(tiles, axis, split_axis=0, concat_axis=0, tiled=True)


def from_everyone(x, axis):
    return exchange(jnp.broadcast_to(x, (lax.axis_size(axis), *x.shape)), axis)


def swapped(x, axis, flip):
    return lax.ppermute(x, axis, [(i, i ^ flip) for i in range(lax.axis_size(axis))])


def in_two_parts(x):
    first = lax.reduce_precision(x, 8, 7)
    return jnp.concatenate([first, x - first], axis=0).astype(jnp.bfloat16)


def doubled(x, axis, flip):
    other = swapped(x, axis, flip)
    high = (lax.axis_index(axis) & flip) != 0
    return jnp.concatenate([jnp.where(high, other, x), jnp.where(high, x, other)], axis=0)


def tied(*values):
    return lax.optimization_barrier(values)


def summed(tiles):
    return tiles.astype(jnp.float32).sum(axis=0)


def forward_kernel(ids_ref, near_ref, far_ref, proj_ref, lcb_ref, *refs):
    emb_ref, normed_ref, inv_ref, lcb_sum_ref, table_ref, even_ref, odd_ref, fm_ref = refs[-8:]
    rank, n_emb = proj_ref.shape
    half, width = near_ref.shape

    @pl.when(pl.program_id(0) == 0)
    def _():
        lcb_sum_ref[...] = jnp.zeros_like(lcb_sum_ref)

        @pl.loop(0, half // 128)
        def _(i):
            at = pl.multiple_of(i * 128, 128)
            table_ref[pl.ds(at, 128), :] = near_ref[pl.ds(at, 128), :].astype(jnp.float32)
            table_ref[pl.ds(half + at, 128), :] = far_ref[pl.ds(at, 128), :].astype(jnp.float32)

    proj = proj_ref[...]
    scale = 1.0 / (rank * n_emb)
    per = normed_ref.shape[2] // n_emb
    outputs = lcb_ref.shape[1]
    lcb_sum = jnp.zeros(lcb_sum_ref.shape, jnp.float32)
    for start in range(0, GROUP, ROWS):
        for e in range(0, ROWS, 2):
            rows_ref = (even_ref, odd_ref)[e // 2 % 2]
            for r in range(2 * n_emb):
                row = ids_ref[start + e + r // n_emb, r % n_emb]
                rows_ref[pl.ds(r, 1), :] = table_ref[pl.ds(row, 1), :]
            pair = rows_ref[...].astype(jnp.bfloat16)
            first, second = pair[:n_emb], pair[n_emb:]
            emb_ref[start + e] = first
            emb_ref[start + e + 1] = second
            compressed = jnp.dot(
                proj, jnp.concatenate([first, second], axis=1), preferred_element_type=jnp.float32
            ).astype(jnp.bfloat16)
            left = jnp.concatenate(
                [compressed[:, :width], compressed[:, width:], lcb_ref[start + e], lcb_ref[start + e + 1]], axis=0
            )
            fm = lax.dot_general(left, pair, (((1,), (1,)), ((), ())), preferred_element_type=jnp.float32)
            fm_ref[pl.ds(e * rank, rank), :] = fm[:rank, :n_emb]
            fm_ref[pl.ds((e + 1) * rank, rank), :] = fm[rank : 2 * rank, n_emb:]
            lcb_sum += fm[2 * rank : 2 * rank + outputs, :n_emb] + fm[2 * rank + outputs :, n_emb:]
        parts = [fm_ref[pl.ds(k, ROWS, stride=rank), :] for k in range(rank)]
        mean = jnp.sum(sum(parts), axis=1, keepdims=True) * scale
        parts = [p - mean for p in parts]
        var = jnp.sum(sum(p * p for p in parts), axis=1, keepdims=True) * scale
        inv = 1.0 / jnp.sqrt(var + 1.0)
        for k in range(rank):
            at = k % per * n_emb
            normed_ref[k // per, start : start + ROWS, at : at + n_emb] = (parts[k] * inv).astype(jnp.bfloat16)
        inv_ref[start : start + ROWS] = jnp.broadcast_to(inv, (ROWS, inv_ref.shape[1]))
    lcb_sum_ref[...] += lcb_sum


def forward_features(ids, near, far, projection, lcb_grad, blocks, start, count, before=()):
    examples, n_emb = ids.shape
    half, width = near.shape
    rank = projection.shape[1]
    columns = rank * n_emb // blocks
    skip = start // GROUP
    outputs = lcb_grad.shape[1]
    return pl.pallas_call(
        forward_kernel,
        grid=(count // GROUP,),
        in_specs=[
            pl.BlockSpec((GROUP, n_emb), lambda g: (g + skip, 0), memory_space=pltpu.SMEM),
            pl.BlockSpec((half, width), lambda g: (0, 0)),
            pl.BlockSpec((half, width), lambda g: (0, 0)),
            pl.BlockSpec((rank, n_emb), lambda g: (0, 0)),
            pl.BlockSpec((GROUP, outputs, width), lambda g: (g + skip, 0, 0)),
            *(pl.BlockSpec(memory_space=pl.ANY) for _ in before),
        ],
        out_specs=[
            pl.BlockSpec((GROUP, n_emb, width), lambda g: (g + skip, 0, 0)),
            pl.BlockSpec((blocks, GROUP, columns), lambda g: (0, g, 0)),
            pl.BlockSpec((GROUP, 128), lambda g: (g + skip, 0)),
            pl.BlockSpec((outputs, n_emb), lambda g: (0, 0)),
        ],
        out_shape=[
            jax.ShapeDtypeStruct((examples, n_emb, width), jnp.bfloat16),
            jax.ShapeDtypeStruct((blocks, count, columns), jnp.bfloat16),
            jax.ShapeDtypeStruct((examples, 128), jnp.float32),
            jax.ShapeDtypeStruct((outputs, n_emb), jnp.float32),
        ],
        scratch_shapes=[
            pltpu.VMEM((2 * half, width), jnp.float32),
            pltpu.VMEM((2 * n_emb, width), jnp.float32),
            pltpu.VMEM((2 * n_emb, width), jnp.float32),
            pltpu.VMEM((ROWS * rank, n_emb), jnp.float32),
        ],
        input_output_aliases={5: 0, 6: 2} if before else {},
        cost_estimate=pl.CostEstimate(
            flops=100_000_000 * count,
            bytes_accessed=half * width * 4 + count * n_emb * width * 2,
            transcendentals=0,
        ),
        name="fm_forward",
    )(ids, near, far, projection.T, lcb_grad, *before)


def backward_kernel(grad_ref, first_ref, last_ref, inv_ref, emb_ref, proj_ref, fm_grad_ref):
    n_emb, rank = proj_ref.shape
    width = emb_ref.shape[2]
    per = last_ref.shape[2] // n_emb
    scale = 1.0 / (rank * n_emb)
    at_last = pl.program_id(0) == pl.num_programs(0) - 1

    @pl.when(pl.program_id(0) == 0)
    def _():
        proj_ref[...] = jnp.zeros_like(proj_ref)

    proj = jnp.zeros(proj_ref.shape, jnp.float32)
    for start in range(0, GROUP, ROWS):
        rows = slice(start, start + ROWS)
        grads = [grad_ref[rows, k * n_emb : (k + 1) * n_emb] for k in range(rank)]
        cuts = [(k // per, rows, slice(k % per * n_emb, (k % per + 1) * n_emb)) for k in range(rank)]
        normed = [
            jnp.where(at_last, last_ref[cut].astype(jnp.float32), first_ref[cut].astype(jnp.float32)) for cut in cuts
        ]
        mean = jnp.sum(sum(grads), axis=1, keepdims=True) * scale
        along = jnp.sum(sum(g * x for g, x in zip(grads, normed)), axis=1, keepdims=True) * scale
        inv = inv_ref[rows, :1]
        for k in range(rank):
            fm_grad_ref[pl.ds(k, ROWS, stride=rank), :] = (grads[k] - mean - normed[k] * along) * inv
        pairs, backs = [], []
        for e in range(0, ROWS, 2):
            fm_grad = fm_grad_ref[pl.ds(e * rank, 2 * rank), :].astype(jnp.bfloat16)
            pair = jnp.concatenate([emb_ref[start + e], emb_ref[start + e + 1]], axis=1)
            back = jnp.dot(fm_grad, pair, preferred_element_type=jnp.float32).astype(jnp.bfloat16)
            pairs.append(pair)
            backs += [back[:rank, :width], back[rank:, width:]]
        proj += lax.dot_general(
            jnp.concatenate(pairs, axis=1),
            jnp.concatenate(backs, axis=1),
            (((1,), (1,)), ((), ())),
            preferred_element_type=jnp.float32,
        )
    proj_ref[...] += proj


def backward_features(normed_grad, normed_first, normed_last, inv_scale, embedded):
    examples, n_emb, width = embedded.shape
    blocks, count, columns = normed_first.shape
    rank = blocks * columns // n_emb
    firsts = count // GROUP
    assert normed_last.shape[1] == GROUP and count + GROUP == examples
    return pl.pallas_call(
        backward_kernel,
        grid=(firsts + 1,),
        in_specs=[
            pl.BlockSpec((GROUP, rank * n_emb), lambda g: (g, 0)),
            pl.BlockSpec((blocks, GROUP, columns), lambda g: (0, jnp.minimum(g, firsts - 1), 0)),
            pl.BlockSpec((blocks, GROUP, columns), lambda g: (0, 0, 0)),
            pl.BlockSpec((GROUP, 128), lambda g: (g, 0)),
            pl.BlockSpec((GROUP, n_emb, width), lambda g: (g, 0, 0)),
        ],
        out_specs=pl.BlockSpec((n_emb, rank), lambda g: (0, 0)),
        out_shape=jax.ShapeDtypeStruct((n_emb, rank), jnp.float32),
        scratch_shapes=[pltpu.VMEM((ROWS * rank, n_emb), jnp.float32)],
        cost_estimate=pl.CostEstimate(
            flops=40_000_000 * examples,
            bytes_accessed=examples * n_emb * (width * 2 + rank * 6),
            transcendentals=0,
        ),
        name="fm_backward",
    )(normed_grad, normed_first, normed_last, inv_scale, embedded)


def both_cores(half, dims, axes):
    other = swapped(half, "c", 1)
    high = lax.axis_index("c") == 1
    both = [h.reshape(*dims, *half.shape[1:]) for h in (half, other)]
    both = jnp.where(high, jnp.stack(both[::-1]), jnp.stack(both))
    return jnp.transpose(both, axes).reshape(-1, *half.shape[1:])


def per_device(feature_ids, emb_table, factor_machine_projection, mlp_weight, momentum, hidden_grad, lcb_grad):
    mp, zl, y, x, c = (lax.axis_size(a) for a in ("mp", "zl", "y", "x", "c"))
    own = emb_table.shape[0]
    examples, hidden = hidden_grad.shape

    to_worker = []
    for block in range(zl * y * x * c):
        cx, zy = divmod(block, zl * y)
        at_c, at_x = divmod(cx, x)
        to_worker.append((block, (zy * x + at_x) * c + at_c))
    to_owner = [(worker, owner) for owner, worker in to_worker]

    width = emb_table.shape[1]
    weights = mlp_weight.astype(jnp.bfloat16)
    table = from_everyone(jnp.concatenate([emb_table, weights[:, :width], weights[:, width:]], axis=0), "y")
    weights = table[:, own:].reshape(y, hidden // width, -1, width)
    weights = jnp.swapaxes(weights, 1, 2).reshape(-1, hidden)
    table = from_everyone(table[:, :own].reshape(-1, width), ("mp", "zl")).reshape(-1, width)
    state = lax.ppermute(jnp.stack([mlp_weight, momentum]), DP, to_worker)
    weight_rows, momentum_rows = state[0], state[1]
    weights = doubled(weights, "zl", 1)
    weights = jnp.broadcast_to(weights, (x, *weights.shape))
    owner, row = lax.div(feature_ids, own), lax.rem(feature_ids, own)
    owner, at_mp = lax.div(owner, mp), lax.rem(owner, mp)
    owner, at_c = lax.div(owner, c), lax.rem(owner, c)
    owner, at_x = lax.div(owner, x), lax.rem(owner, x)
    at_zl, at_y = lax.div(owner, y), lax.rem(owner, y)
    ids = (((((at_c ^ lax.axis_index("c")) * x + at_x) * mp + at_mp) * zl + at_zl) * y + at_y) * own + row
    table = from_everyone(table, "x").reshape(-1, width)
    weights, table = tied(weights, table)
    table_far = swapped(table, "c", 1)
    weights = exchange(weights, "x").reshape(-1, hidden)

    blocks = 2 * c * x
    cut = int(examples * FIRST_SHARE)
    shares = ((0, cut), (cut, examples - cut))
    inputs = (ids, table, table_far, factor_machine_projection, lcb_grad)
    embedded, normed_a, inv_scale, lcb_a = forward_features(*inputs, blocks, *shares[0])
    weights = both_cores(weights, (x, zl, y, mlp_weight.shape[0]), (2, 3, 1, 0, 4, 5))
    embedded, normed_b, inv_scale, lcb_b = forward_features(
        *inputs, blocks, *shares[1], (embedded, inv_scale)
    )
    columns_a = exchange(normed_a.reshape(c * x, 2 * cut, -1), CX)

    tiled_weights = weights.reshape(blocks, -1, hidden)
    preact = jnp.concatenate(
        [
            jnp.einsum("jbk,jkn->bn", normed, tiled_weights, preferred_element_type=jnp.float32)
            for normed in (normed_a, normed_b)
        ],
        axis=0,
    )
    sigmoid_pre = jax.nn.sigmoid(preact)
    preact_grad = (
        hidden_grad.astype(jnp.float32) * sigmoid_pre * (1.0 + preact * (1.0 - sigmoid_pre))
    ).astype(jnp.bfloat16)
    group_grad = exchange(
        jnp.concatenate(
            [
                jnp.broadcast_to(preact_grad, (c * x, examples, hidden)),
                normed_b.reshape(c * x, -1, hidden),
            ],
            axis=1,
        ),
        CX,
    )

    normed_part = lax.dot_general(preact_grad, weights, (((1,), (1,)), ((), ())), preferred_element_type=jnp.float32)
    proj_part = backward_features(normed_part, normed_a, normed_b, inv_scale, embedded)
    (start_a, count_a), (start_b, count_b) = shares
    weight_grad = jnp.concatenate(
        [
            sum(
                jnp.einsum(
                    "sbk,sbn->kn",
                    part[:, at : at + count],
                    group_grad[:, start : start + count],
                    preferred_element_type=jnp.float32,
                )
                for part, at, start, count in (
                    (columns_a, half * count_a, start_a, count_a),
                    (group_grad, examples + half * count_b, start_b, count_b),
                )
            )
            for half in range(2)
        ],
        axis=0,
    )
    arrived = exchange(weight_grad.astype(jnp.bfloat16).reshape(zl * y, -1, hidden), ZY)
    small = proj_part.T
    small += swapped(small, "mp", 1)
    small += swapped(small, "mp", 3)
    small = jnp.concatenate([small, lcb_a + lcb_b], axis=1)
    arrived, small = tied(arrived, small)
    new_momentum = 0.9 * momentum_rows + summed(arrived)
    new_weight = weight_rows - 0.01 * new_momentum
    own_rows = new_weight.shape[0]
    arrived = from_everyone(jnp.concatenate([new_weight, small], axis=0).astype(jnp.bfloat16), ZY)
    next_weight = arrived[:, :own_rows].reshape(-1, hidden)
    small = in_two_parts(summed(arrived[:, own_rows:]))
    column_rows = next_weight.shape[0]
    arrived = from_everyone(jnp.concatenate([next_weight, small], axis=0), "x")
    state = lax.ppermute(jnp.stack([new_weight, new_momentum]), DP, to_owner)
    arrived, state = tied(arrived, state)
    other = swapped(arrived, "c", 1)
    high = lax.axis_index("c") == 1
    halves = [h[:, :column_rows] for h in (arrived, other)]
    next_weight = jnp.where(high, jnp.stack(halves[::-1]), jnp.stack(halves)).reshape(-1, hidden)
    small = [summed(h[:, column_rows:].reshape(2 * x, -1, hidden)) for h in (arrived, other)]
    small = small[0] + small[1]
    n_emb = small.shape[1] // 2
    return (state[0], state[1], next_weight, small[:, :n_emb].T, small[:, n_emb:].T)


def solution(mesh):
    torus = Mesh(mesh.devices.reshape(2, 8, 4, 2, mesh.shape["mp"]), DP_MP)
    placed = (
        P(DP, None),
        P(DP_MP, None),
        P(),
        P(DP, "mp"),
        P(DP, "mp"),
        P(DP, "mp"),
        P(DP, "mp", None),
    )

    return jax.shard_map(
        per_device,
        mesh=torus,
        in_specs=placed,
        out_specs=(P(DP, "mp"), P(DP, "mp"), P(None, "mp"), P(), P(None, "mp")),
        check_vma=False,
    )
```
